256 devices in a mesh: gx: 16 (over y_lo, z), gy: 16 (over y_hi, x, core).
Axes of the slice: x: 4, y: 4 (y_hi: 2, y_lo: 2; y = y_hi * 2 + y_lo), z: 8, core: 2. Of those that a mesh axis runs over, the one named last changes fastest.
Arguments:
- wide_index: int32 [4, 32, 2048], replicated, may hold values from 0 to 131071
- wide_table: bfloat16 [4, 131072, 256], P(None, ('gx', 'gy')), may hold values from -1.09375 to 1.09375
- wide_proj: bfloat16 [4, 256, 128], replicated, may hold values from -0.375 to 0.375
- thin_index: int32 [8, 32, 2048], P(None, None, 'gx'), may hold values from 0 to 65535
- thin_table: bfloat16 [8, 32, 65536], P(None, None, 'gy'), may hold values from -1.09375 to 1.09375
- thin_proj: bfloat16 [8, 32, 128], replicated, may hold values from -1 to 1
Outputs:
- wide_out: float32 [2048, 512], P(('gx', 'gy'))
- thin_out: float32 [2048, 1024], P(('gx', 'gy'))
The draws below stay inside these ranges and needn't reach their ends.
All inputs are finite; a program needn't handle non-finite values.
Results may differ from the reference program's by a relative error of at most 0.0003.
Values sent between devices are 32-bit elements; how exact they have to be, the bound alone decides.
A program may use at most 64 MiB of HBM per device.

```python
import math
import jax
import jax.numpy as jnp
import numpy as np
from jax import lax

TW = 4
TT = 8
WW = 256
WT = 32
PROJ = 128
L = 32
RW_DEV = 512
RT_DEV = 4096
BAGS = 2048
ROWS_W = 131072
ROWS_T = 65536
N_GX = 16
N_GY = 16


def with_ends(array, key, least, largest):
    longest = array.shape.index(max(array.shape))
    spots = []
    for shift in (0, 1):
        where = [jax.random.randint(jax.random.fold_in(key, axis), (), 0, length) for axis, length in enumerate(array.shape)]
        where[longest] = (where[longest] + shift) % array.shape[longest]
        spots.append(tuple(where))
    return array.at[spots[0]].set(least).at[spots[1]].set(largest)


def level_of(rng, extent, pieces, low, top_value):
    level = 1.0
    for dim, blocks in pieces:
        draws = jax.random.uniform(jax.random.fold_in(jax.random.fold_in(rng, 6), dim), (blocks,), jnp.float32, low / len(pieces), top_value / len(pieces))
        level = level * jnp.repeat(jnp.exp(draws), extent[dim] // blocks).reshape((-1,) + (1,) * (len(extent) - 1 - dim))
    return level


def cumulative_ranks(count, lean):
    portions = [(1 << 20) // math.isqrt(standing ** lean) + 1 for standing in range(1, count + 1)]
    width = 1 + sum(portions) // (1 << 30)
    return np.cumsum(np.array([max(1, weight // width) for weight in portions]))


def ranked_ids(rng, extent, number_of, lean):
    listing = cumulative_ranks(number_of, lean)
    pick = jax.random.randint(jax.random.fold_in(rng, 1), extent, 0, int(listing[number_of - 1]))
    grade = jnp.searchsorted(jnp.asarray(listing, jnp.int32), pick, side="right")
    return jax.random.permutation(jax.random.fold_in(rng, 2), number_of)[grade].astype(jnp.int32)


def skewed_wide(rng, shape, number_of, lean):
    loads = [min(1 << octave, number_of + 1 - (1 << octave)) * (1 << 20) // math.isqrt((1 << octave) ** lean) + 1 for octave in range((number_of + 1).bit_length()) if 1 << octave <= number_of]
    deviation = 1 + sum(loads) // (1 << 30)
    listing = np.cumsum(np.array([max(1, weight // deviation) for weight in loads]))
    ticket = jax.random.randint(jax.random.fold_in(rng, 1), shape, 0, int(listing[len(loads) - 1]))
    start = jnp.left_shift(1, jnp.searchsorted(jnp.asarray(listing, jnp.int32), ticket, side="right").astype(jnp.int32))
    rank = start - 1 + jax.random.randint(jax.random.fold_in(rng, 4), shape, 0, 1 << 30) % jnp.minimum(start, number_of + 1 - start)
    return jax.random.permutation(jax.random.fold_in(rng, 2), number_of)[rank].astype(jnp.int32)


def noise(key, shape, spread, limit, pieces=(), held_as=jnp.bfloat16):
    drawn = jax.random.normal(key, shape, jnp.float32) * spread
    if len(pieces) > 0:
        drawn = level_of(key, shape, pieces, -0.22, 0.18) * drawn
    return jnp.clip(drawn, min=-limit, max=limit).astype(held_as)


def setup_inputs(seed: int = 0) -> dict:
    seeds = jax.random.split(jax.random.key(seed), 7)
    wide_index = with_ends(skewed_wide(seeds[0], (TW, L, BAGS), RW_DEV * N_GX * N_GY, 1), jax.random.fold_in(seeds[0], 3), 0, (RW_DEV * N_GX * N_GY) - 1).astype(jnp.int32)
    wide_table = noise(seeds[1], (TW, ROWS_W, WW), 0.18, 1.09375, ((1, 256),))
    wide_proj = noise(seeds[2], (TW, WW, PROJ), WW ** -0.5, 0.375)
    thin_index = with_ends(ranked_ids(seeds[3], (TT, L, BAGS), RT_DEV * N_GY, 1), jax.random.fold_in(seeds[3], 3), 0, (RT_DEV * N_GY) - 1).astype(jnp.int32)
    thin_table = noise(seeds[4], (TT, WT, ROWS_T), 0.18, 1.09375, ((2, 16),))
    thin_proj = noise(seeds[5], (TT, WT, PROJ), WT ** -0.5, 1.0)
    return {"wide_index": wide_index, "wide_table": wide_table, "wide_proj": wide_proj, "thin_index": thin_index, "thin_table": thin_table, "thin_proj": thin_proj}


def reference(wide_index, wide_table, wide_proj, thin_index, thin_table, thin_proj):
    wide_parts = []
    for which in range(TW):
        gathered = jnp.take(wide_table[which], wide_index[which], axis=0).astype(jnp.float32)
        pooled = jnp.sum(gathered, axis=0)
        wide_parts.append(jnp.dot(pooled, wide_proj[which].astype(jnp.float32), precision=lax.Precision.HIGHEST))
    thin_parts = []
    for which in range(TT):
        gathered = jnp.take(thin_table[which], thin_index[which], axis=1).astype(jnp.float32)
        pooled = jnp.sum(gathered, axis=1).T
        thin_parts.append(jnp.dot(pooled, thin_proj[which].astype(jnp.float32), precision=lax.Precision.HIGHEST))
    wide_out = jnp.concatenate(wide_parts, axis=1)
    thin_out = jnp.concatenate(thin_parts, axis=1)
    return (wide_out, thin_out)
```

```python
import jax
import jax.numpy as jnp
from jax import lax
from jax.experimental import pallas as pl
from jax.experimental.pallas import tpu as pltpu
from jax.sharding import PartitionSpec as P

F32, BF16, I32 = jnp.float32, jnp.bfloat16, jnp.int32
MESH = pl.DeviceIdType.MESH
GX_GY = ("gx", "gy")

WIDE_SLOTS = 2
THIN_SLOTS = 8
BLOCK = 256


def keys_of(index, first, count):
    row = index - first
    place = lax.broadcasted_iota(I32, row.shape, 0)
    return jnp.where((row >= 0) & (row < count), row * 32 + place, -1)


def next_slot(keys, slot):
    return jnp.max(jnp.where(keys < slot, keys, -1), axis=0, keepdims=True)


def tiled_row(values, rows):
    return jnp.broadcast_to(values, (rows, values.shape[1]))


def pool_kernel(wi, wt, wp, ti, tt, wide, thin, ids, keys, hits, proj, lines, low, sums):
    t = pl.program_id(0)
    gx, gy = lax.axis_index("gx"), lax.axis_index("gy")
    me = gx * 16 + gy
    rows_w = wt.shape[1]
    one, zero = jnp.ones((16, 128), BF16), jnp.zeros((16, 128), BF16)

    @pl.when(t == 0)
    def _():
        ids[...] = (lax.broadcasted_iota(I32, ids.shape, 0) - 256).astype(F32).astype(BF16)

    projected = jnp.dot(wt[0], wp[0], preferred_element_type=F32).T
    high = projected.astype(BF16)
    proj[:128] = high
    proj[128:] = (projected - high.astype(F32)).astype(BF16)

    all_keys = keys_of(wi[0], me * rows_w, rows_w)
    keys[...] = all_keys
    slots = [jnp.max(all_keys, axis=0, keepdims=True)]
    for _ in range(WIDE_SLOTS):
        slots.append(next_slot(all_keys, slots[-1]))

    def wide_id(slot):
        return tiled_row(jnp.where(slot < 0, 256, (slot >> 5) - 256).astype(F32), 16).astype(BF16)

    blocks = all_keys.shape[1] // BLOCK
    more = [jnp.max(slots[WIDE_SLOTS][:, b * BLOCK : (b + 1) * BLOCK]) for b in range(blocks)]
    for b in range(blocks):
        for c in range(BLOCK // 128):
            at = b * BLOCK + c * 128
            marks = [wide_id(s[:, at : at + 128]) for s in slots[:WIDE_SLOTS]]
            for r in range(rows_w // 16):
                here = ids[r * 16 : r * 16 + 16, :]
                hit = jnp.where(here == marks[0], one, zero)
                for mark in marks[1:]:
                    hit = hit + jnp.where(here == mark, one, zero)
                hits[r * 16 : r * 16 + 16, at : at + 128] = hit
    for b in range(blocks):

        @pl.when(more[b] >= 0)
        def _(b=b):
            block = slice(b * BLOCK, (b + 1) * BLOCK)

            def body(carry):
                slot, _ = carry
                for c in range(BLOCK // 128):
                    at = b * BLOCK + c * 128
                    mark = wide_id(slot[:, c * 128 : c * 128 + 128])
                    for r in range(rows_w // 16):
                        here = ids[r * 16 : r * 16 + 16, :]
                        spot = (slice(r * 16, r * 16 + 16), slice(at, at + 128))
                        hits[spot] = hits[spot] + jnp.where(here == mark, one, zero)
                slot = next_slot(keys[:, block], slot)
                return slot, jnp.max(slot)

            lax.while_loop(lambda carry: carry[1] >= 0, body, (slots[WIDE_SLOTS][:, block], more[b]))

    step = [(8 >> ((d - t + 4) % 4)) * 8 for d in range(4)]
    for b in range(blocks):
        both = jnp.dot(proj[...], hits[:, b * BLOCK : (b + 1) * BLOCK], preferred_element_type=F32)
        found = (both[:128] + both[128:]).T
        for g in range(BLOCK // 128):
            y_lo, z = divmod(b * (BLOCK // 128) + g, 8)
            for y_hi in range(2):
                for x in range(4):
                    bits = ((x // 2) ^ (x % 2), y_hi ^ y_lo, x // 2, y_hi)
                    place = sum((s for s, bit in zip(step, bits) if bit), z)
                    for core in range(2):
                        at = g * 128 + y_hi * 64 + x * 16 + core * 8
                        wide[0, core * 128 + place] = found[at : at + 8]

    rows_t = tt.shape[2]
    groups = rows_t // 256
    last = []
    for i in range(2):
        for g in range(groups):
            lines[i, g * 32 : g * 32 + 32, :] = tt[i, :, g * 256 : g * 256 + 256]
        thin_keys = keys_of(ti[i], gy * rows_t, rows_t)
        slot = jnp.max(thin_keys, axis=0, keepdims=True)
        taken = [slot]
        for _ in range(THIN_SLOTS):
            taken.append(next_slot(thin_keys, taken[-1]))
        last.append((thin_keys, taken[-1], jnp.max(taken[-1])))

        def mark_low(slot, at):
            mark = tiled_row(((slot >> 5) & 255).astype(F32), 16).astype(BF16)
            for r in range(16):
                here = ids[256 + r * 16 : 272 + r * 16, :]
                low[i, r * 16 : r * 16 + 16, at : at + 128] = jnp.where(here == mark, one, zero)

        def select(slot, found, total):
            group = tiled_row(slot >> 13, 8)
            picked = [jnp.zeros((8, 128), F32)] * 4
            for g in range(groups):
                same = group == g
                picked = [
                    jnp.where(same, found[g * 32 + f * 8 : g * 32 + f * 8 + 8], picked[f])
                    for f in range(4)
                ]
            return [a + b for a, b in zip(total, picked)]

        for k in range(THIN_SLOTS):
            mark_low(taken[k], k * 128)
        total = [jnp.zeros((8, 128), F32)] * 4
        for pair in range(THIN_SLOTS // 2):
            found = jnp.dot(
                lines[i], low[i, :, pair * 256 : pair * 256 + 256], preferred_element_type=F32
            )
            for k in range(2):
                total = select(taken[pair * 2 + k], found[:, k * 128 : k * 128 + 128], total)
        base = (t % 2) * 64 + i * 32
        for f in range(4):
            sums[pl.ds(pl.multiple_of(base + f * 8, 8), 8), :] = total[f]

    for i in range(2):
        thin_keys, slot, top = last[i]

        @pl.when(top >= 0)
        def _(i=i, slot=slot, top=top):
            base = (t % 2) * 64 + i * 32
            again = keys_of(ti[i], gy * rows_t, rows_t)

            def body(carry):
                slot, _ = carry
                mark = tiled_row(((slot >> 5) & 255).astype(F32), 16).astype(BF16)
                for r in range(16):
                    here = ids[256 + r * 16 : 272 + r * 16, :]
                    low[i, r * 16 : r * 16 + 16, :128] = jnp.where(here == mark, one, zero)
                found = jnp.dot(lines[i], low[i, :, :128], preferred_element_type=F32)
                group = tiled_row(slot >> 13, 8)
                for f in range(4):
                    spot = pl.ds(pl.multiple_of(base + f * 8, 8), 8)
                    total = sums[spot, :]
                    for g in range(groups):
                        piece = found[g * 32 + f * 8 : g * 32 + f * 8 + 8]
                        total = total + jnp.where(group == g, piece, 0.0)
                    sums[spot, :] = total
                slot = next_slot(again, slot)
                return slot, jnp.max(slot)

            lax.while_loop(lambda carry: carry[1] >= 0, body, (slot, top))

    @pl.when(t % 2 == 1)
    def _():
        thin[0] = sums[...].T


def pool(wide_index, wide_table, wide_proj, thin_index, thin_table):
    tw, depth, bags = wide_index.shape
    rows_w, ww = wide_table.shape[1:]
    per_step = thin_index.shape[0] // tw
    own_bags = thin_index.shape[2]
    wt, rows_t = thin_table.shape[1:]

    def block(shape):
        return pl.BlockSpec(shape, lambda t: (t, 0, 0))

    return pl.pallas_call(
        pool_kernel,
        grid=(tw,),
        in_specs=[
            block((1, depth, bags)),
            block((1, rows_w, ww)),
            block((1, ww, 128)),
            block((per_step, depth, own_bags)),
            block((per_step, wt, rows_t)),
        ],
        out_specs=[
            pl.BlockSpec((1, bags // 8, 8, 128), lambda t: (t, 0, 0, 0)),
            pl.BlockSpec((1, 128, 128), lambda t: (t // 2, 0, 0)),
        ],
        out_shape=[
            jax.ShapeDtypeStruct((tw, bags // 8, 8, 128), F32),
            jax.ShapeDtypeStruct((2, 128, 128), F32),
        ],
        scratch_shapes=[
            pltpu.VMEM((rows_w, 128), BF16),
            pltpu.VMEM((depth, bags), I32),
            pltpu.VMEM((rows_w, bags), BF16),
            pltpu.VMEM((256, rows_w), BF16),
            pltpu.VMEM((2, rows_t // 256 * wt, 256), BF16),
            pltpu.VMEM((2, 256, THIN_SLOTS * 128), BF16),
            pltpu.VMEM((128, 128), F32),
        ],
        compiler_params=pltpu.CompilerParams(dimension_semantics=("arbitrary",)),
    )(wide_index, wide_table, wide_proj, thin_index, thin_table)


def exchange_kernel(
    w, th, pj, wide_out, thin_out, own, r0, r1, r2, r3, r4, rz, rt,
    load, ssem, rsem, zs, zr, ts, tr,
):
    gx, gy = lax.axis_index("gx"), lax.axis_index("gy")
    y_lo, z = gx // 8, gx % 8
    y_hi, x, core = gy // 8, (gy // 2) % 4, gy % 2

    def gy_of(y_hi, x, core):
        return y_hi * 8 + x * 2 + core

    links = [
        ((gx, gy_of(y_hi, x + 1 - 2 * (x % 2), core)), (x // 2 + x % 2) % 2),
        (((1 - y_lo) * 8 + z, gy), (y_hi + y_lo) % 2),
        ((gx, gy_of(y_hi, 3 - x, core)), x // 2),
        (((1 - y_lo) * 8 + z, gy_of(1 - y_hi, x, core)), y_hi),
    ]
    other = (gx, gy_of(y_hi, x, 1 - core))
    along_z = [None] + [(y_lo * 8 + (z + d) % 8, gy) for d in range(1, 8)]
    along_gy = [None] + [(gx, (gy + d) % 16) for d in range(1, 16)]

    barrier = pltpu.get_barrier_semaphore()
    peers = along_gy[1:] + along_z[1:] + [links[1][0], links[3][0]]
    for peer in peers:
        pl.semaphore_signal(barrier, inc=1, device_id=peer, device_id_type=MESH)
    loads = []
    for c in range(4):
        loads.append(pltpu.make_async_copy(w.at[c, core], own.at[c], load.at[c]))
        loads[-1].start()
    pl.semaphore_wait(barrier, len(peers))

    def send(src, dst, s, r, to):
        copy = pltpu.make_async_remote_copy(
            src_ref=src, dst_ref=dst, send_sem=s, recv_sem=r, device_id=to, device_id_type=MESH
        )
        copy.start()
        return copy

    sends = []
    halves = []
    for c in range(4):
        halves.append(send(w.at[c, 1 - core], r0.at[c], ssem.at[0, c], rsem.at[0, c], other))
    thins = []
    for d in range(1, 16):
        thins.append(send(th.at[:, along_gy[d][1]], rt.at[d], ts.at[d], tr.at[d], along_gy[d]))

    held, got = [own.at[c] for c in range(4)], halves
    landed = [r0, r1, r2, r3, r4]
    bits = [[links[(c + k) % 4][1] for k in range(4)] for c in range(4)]
    partners = [[links[(c + k) % 4][0] for k in range(4)] for c in range(4)]

    def thin_part():
        for copy in thins:
            copy.wait_recv()
        pooled = th[:, gy]
        for d in range(1, 16):
            pooled = pooled + rt[d]
        group = lax.broadcasted_iota(I32, (8, 128), 1) // 32
        for h in range(2):
            parts = [jnp.where(group == g, pooled[h], 0.0) for g in range(4)]
            out = jnp.dot(
                jnp.concatenate(parts, axis=0),
                pj[h].astype(F32),
                preferred_element_type=F32,
                precision=lax.Precision.HIGHEST,
            )
            for g in range(4):
                at = (h * 4 + g) * 128
                thin_out[:, at : at + 128] = out[g * 8 : g * 8 + 8]

    for k in range(5):
        nxt = []
        for c in range(4):
            got[c].wait_recv()
            sends.append(got[c])
            new = landed[k]
            if k == 0:
                loads[c].wait()
            kept = bits[c][k - 1] if k > 0 else None
            if k < 4:
                go, stay = 1 - bits[c][k], bits[c][k]
                for part in (go, stay):
                    if k == 0:
                        own[c, part] = own[c, part] + r0[c, part]
                    elif k == 1:
                        new[c, part] = new[c, part] + own[c, kept, part]
                    else:
                        new[c, part] = new[c, part] + landed[k - 1][c, kept, part]
                    if part is go:
                        source = own if k == 0 else new
                        nxt.append(
                            send(
                                source.at[c, go],
                                landed[k + 1].at[c],
                                ssem.at[k + 1, c],
                                rsem.at[k + 1, c],
                                partners[c][k],
                            )
                        )
            else:
                new[c] = new[c] + landed[k - 1][c, kept]
        got = nxt
        if k == 0:
            thin_part()

    lasts = []
    for d in range(1, 8):
        lasts.append(
            send(r4.at[:, (z + d) % 8], rz.at[d], zs.at[d], zr.at[d], along_z[d])
        )
    total = r4[:, z]
    for d in range(1, 8):
        lasts[d - 1].wait_recv()
        total = total + rz[d]
    for c in range(4):
        wide_out[:, c * 128 : c * 128 + 128] = total[c]
    for copy in sends + lasts + thins:
        copy.wait_send()


def exchange(wide, thin, thin_proj):
    wide = wide.reshape(4, 2, 2, 2, 2, 2, 8, 8, 128)
    thin = thin.reshape(2, 16, 8, 128)
    proj = thin_proj.reshape(2, 128, 128)
    vmem = pl.BlockSpec(memory_space=pltpu.VMEM)
    dma = pltpu.SemaphoreType.DMA
    return pl.pallas_call(
        exchange_kernel,
        in_specs=[pl.BlockSpec(memory_space=pl.ANY), vmem, vmem],
        out_specs=[vmem, vmem],
        out_shape=[
            jax.ShapeDtypeStruct((8, 512), F32),
            jax.ShapeDtypeStruct((8, 1024), F32),
        ],
        scratch_shapes=[
            pltpu.VMEM((4, 2, 2, 2, 2, 8, 8, 128), F32),
            pltpu.VMEM((4, 2, 2, 2, 2, 8, 8, 128), F32),
            pltpu.VMEM((4, 2, 2, 2, 8, 8, 128), F32),
            pltpu.VMEM((4, 2, 2, 8, 8, 128), F32),
            pltpu.VMEM((4, 2, 8, 8, 128), F32),
            pltpu.VMEM((4, 8, 8, 128), F32),
            pltpu.VMEM((8, 4, 8, 128), F32),
            pltpu.VMEM((16, 2, 8, 128), F32),
            dma((4,)),
            dma((5, 4)),
            dma((5, 4)),
            dma((8,)),
            dma((8,)),
            dma((16,)),
            dma((16,)),
        ],
        compiler_params=pltpu.CompilerParams(collective_id=0, has_side_effects=True),
    )(wide, thin, proj)


def local(wide_index, wide_table, wide_proj, thin_index, thin_table, thin_proj):
    wide, thin = pool(wide_index, wide_table, wide_proj, thin_index, thin_table)
    return exchange(wide, thin, thin_proj)


def solution(mesh):
    placed = (P(), P(None, GX_GY, None), P(), P(None, None, "gx"), P(None, None, "gy"), P())
    return jax.shard_map(
        local,
        mesh=mesh,
        in_specs=placed,
        out_specs=(P(GX_GY, None), P(GX_GY, None)),
        check_vma=False,
    )
```

```python
import jax
import jax.numpy as jnp
from jax import lax
from jax.experimental import pallas as pl
from jax.experimental.pallas import tpu as pltpu
from jax.sharding import PartitionSpec as P

F32, BF16, I32 = jnp.float32, jnp.bfloat16, jnp.int32
MESH = pl.DeviceIdType.MESH
GX_GY = ("gx", "gy")

WIDE_SLOTS = 4
THIN_SLOTS = 12
BLOCK = 256


def keys_of(index, first, count, axis):
    row = index - first
    place = lax.broadcasted_iota(I32, row.shape, axis)
    return jnp.where((row >= 0) & (row < count), row * 32 + place, -1)


def next_slot(keys, slot, axis=0):
    return jnp.max(jnp.where(keys < slot, keys, -1), axis=axis, keepdims=True)


def mark_of(values):
    return jnp.broadcast_to(values, (16, values.shape[1])).astype(BF16)


def wide_mark(slot):
    return jnp.where(slot < 0, 256, (slot >> 5) - 256).astype(F32)


def ids_of(first):
    return (lax.broadcasted_iota(I32, (16, 128), 0) + first).astype(F32).astype(BF16)


def one_hot(marks, chunk):
    one, zero = jnp.ones((16, 128), BF16), jnp.zeros((16, 128), BF16)
    hit = jnp.where(chunk == marks[0], one, zero)
    for mark in marks[1:]:
        hit = hit + jnp.where(chunk == mark, one, zero)
    return hit


def split_projection(table, weight):
    projected = jnp.dot(table, weight, preferred_element_type=F32).T
    high = projected.astype(BF16)
    low = (projected - high.astype(F32)).astype(BF16)
    return jnp.concatenate([high, low], axis=0)


def place_of(c, y_lo, z, y_hi, x):
    bits = ((x // 2) ^ (x % 2), y_hi ^ y_lo, x // 2, y_hi)
    return sum((8 >> ((d - c + 4) % 4)) * 8 * bits[d] for d in range(4)) + z


def find_kernel(
    wi, ti, wt, wp, tt, wslot, tslot, wextra, textra,
    wkeys, more, hits, proj, extra, wbuf, pbuf, tbuf, lines, low, zsem, sem,
):
    gx, gy = lax.axis_index("gx"), lax.axis_index("gy")
    tables, _, bags = wi.shape
    rows_w, rows_t = wt.shape[1], tt.shape[2]
    first_w, first_t = (gx * 16 + gy) * rows_w, gy * rows_t
    blocks = bags // BLOCK

    extra[...] = jnp.zeros_like(extra)
    fills = [pltpu.make_async_copy(extra, wextra.at[t], zsem.at[t]) for t in range(tables)]
    for fill in fills:
        fill.start()
    textra[...] = jnp.zeros_like(textra)

    left = jnp.full((1, 128), -1, I32)
    for t in range(tables):
        for b in range(blocks):
            at = slice(b * BLOCK, (b + 1) * BLOCK)
            keys = keys_of(wi[t, :, at], first_w, rows_w, 0)
            slot = jnp.max(keys, axis=0, keepdims=True)
            for k in range(WIDE_SLOTS):
                wslot[t, k : k + 1, at] = wide_mark(slot)
                slot = next_slot(keys, slot)
            more[t, :, at] = slot
            for c in range(BLOCK // 128):
                left = jnp.maximum(left, slot[:, c * 128 : c * 128 + 128])
    wide_left = jnp.max(left)

    thin_keys = keys_of(ti[...], first_t, rows_t, 1)
    slot = jnp.max(thin_keys, axis=1, keepdims=True)
    for k in range(THIN_SLOTS):
        tslot[:, k : k + 1, :] = slot >> 5
        slot = next_slot(thin_keys, slot, 1)
    thin_left = jnp.max(slot)
    for fill in fills:
        fill.wait()

    def fetch(src, dst):
        copy = pltpu.make_async_copy(src, dst, sem)
        copy.start()
        copy.wait()

    @pl.when(wide_left >= 0)
    def _():
        wkeys[...] = keys_of(wi[...], first_w, rows_w, 1)

        def table(t, _):
            @pl.when(jnp.max(more[t]) >= 0)
            def _():
                fetch(wt.at[t], wbuf)
                fetch(wp.at[t], pbuf)
                proj[...] = split_projection(wbuf[...], pbuf[...])

                def block(b, _):
                    at = pl.ds(pl.multiple_of(b * BLOCK, BLOCK), BLOCK)
                    top = jnp.max(more[t, :, at])

                    @pl.when(top >= 0)
                    def _():
                        hits[...] = jnp.zeros_like(hits)

                        def body(carry):
                            slot, _ = carry
                            for c in range(BLOCK // 128):
                                mark = mark_of(wide_mark(slot[:, c * 128 : c * 128 + 128]))
                                for r in range(rows_w // 16):
                                    spot = (slice(r * 16, r * 16 + 16), slice(c * 128, c * 128 + 128))
                                    hits[spot] = hits[spot] + one_hot([mark], ids_of(r * 16 - 256))
                            slot = next_slot(wkeys[t, :, at], slot)
                            return slot, jnp.max(slot)

                        lax.while_loop(lambda carry: carry[1] >= 0, body, (more[t, :, at], top))
                        both = jnp.dot(proj[...], hits[...], preferred_element_type=F32)
                        found = (both[:128] + both[128:]).T
                        step = [(8 >> ((d - t + 4) % 4)) * 8 for d in range(4)]
                        for g in range(BLOCK // 128):
                            group = b * (BLOCK // 128) + g
                            y_lo, z = group // 8, group % 8
                            for y_hi in range(2):
                                crossed = (y_hi + y_lo) % 2
                                for x in range(4):
                                    place = z + step[0] * ((x // 2) ^ (x % 2)) + step[1] * crossed
                                    place = place + step[2] * (x // 2) + step[3] * y_hi
                                    for core in range(2):
                                        row = g * 128 + y_hi * 64 + x * 16 + core * 8
                                        extra[core * 128 + place] = found[row : row + 8]

                    return 0

                lax.fori_loop(0, blocks, block, 0)
                fetch(extra, wextra.at[t])
                extra[...] = jnp.zeros_like(extra)

            return 0

        lax.fori_loop(0, tables, table, 0)

    @pl.when(thin_left >= 0)
    def _():
        groups = rows_t // 256

        def table(i, _):
            keys = keys_of(ti[i], first_t, rows_t, 0)
            slot = jnp.max(keys, axis=0, keepdims=True)
            for _ in range(THIN_SLOTS):
                slot = next_slot(keys, slot)
            top = jnp.max(slot)

            @pl.when(top >= 0)
            def _():
                fetch(tt.at[i], tbuf)
                for g in range(groups):
                    lines[g * 32 : g * 32 + 32, :] = tbuf[:, g * 256 : g * 256 + 256]

                def body(carry):
                    slot, _ = carry
                    mark = mark_of(((slot >> 5) & 255).astype(F32))
                    for r in range(16):
                        low[r * 16 : r * 16 + 16, :] = one_hot([mark], ids_of(r * 16))
                    found = jnp.dot(lines[...], low[...], preferred_element_type=F32)
                    group = jnp.broadcast_to(slot >> 13, (32, 128))
                    total = textra[i]
                    for g in range(groups):
                        total = total + jnp.where(group == g, found[g * 32 : g * 32 + 32], 0.0)
                    textra[i] = total
                    slot = next_slot(keys, slot)
                    return slot, jnp.max(slot)

                lax.while_loop(lambda carry: carry[1] >= 0, body, (slot, top))

            return 0

        lax.fori_loop(0, ti.shape[0], table, 0)


def find(wide_index, thin_index, wide_table, wide_proj, thin_table):
    tw, _, bags = wide_index.shape
    tt, _, own_bags = thin_index.shape
    rows_w, ww = wide_table.shape[1:]
    wt, rows_t = thin_table.shape[1:]
    vmem, anywhere = pl.BlockSpec(memory_space=pltpu.VMEM), pl.BlockSpec(memory_space=pl.ANY)
    return pl.pallas_call(
        find_kernel,
        in_specs=[vmem, vmem, anywhere, anywhere, anywhere],
        out_specs=[vmem, vmem, anywhere, vmem],
        out_shape=[
            jax.ShapeDtypeStruct((tw, WIDE_SLOTS, bags), F32),
            jax.ShapeDtypeStruct((tt, THIN_SLOTS, own_bags), I32),
            jax.ShapeDtypeStruct((tw, bags // 8, 8, 128), F32),
            jax.ShapeDtypeStruct((tt, wt, own_bags), F32),
        ],
        scratch_shapes=[
            pltpu.VMEM(wide_index.shape, I32),
            pltpu.VMEM((tw, 1, bags), I32),
            pltpu.VMEM((rows_w, BLOCK), BF16),
            pltpu.VMEM((256, rows_w), BF16),
            pltpu.VMEM((bags // 8, 8, 128), F32),
            pltpu.VMEM((rows_w, ww), BF16),
            pltpu.VMEM((ww, 128), BF16),
            pltpu.VMEM((wt, rows_t), BF16),
            pltpu.VMEM((rows_t // 256 * wt, 256), BF16),
            pltpu.VMEM((256, 128), BF16),
            pltpu.SemaphoreType.DMA((tw,)),
            pltpu.SemaphoreType.DMA,
        ],
        compiler_params=pltpu.CompilerParams(),
    )(wide_index, thin_index, wide_table, wide_proj, thin_table)


def pool_kernel(
    wslot, tslot, textra, pj, wextra, wt, wp, tt, out,
    part, wbuf, pbuf, tbuf, sums, th, r0, r1, r2, rm, r4, rz, rt,
    esem, wsem, psem, tsem, ssem, rsem, ms, mr, zs, zr, ts, tr,
):
    gx, gy = lax.axis_index("gx"), lax.axis_index("gy")
    y_lo, z = gx // 8, gx % 8
    y_hi, x, core = gy // 8, (gy // 2) % 4, gy % 2

    def device(flip_lo, y_hi, x, core=core):
        return ((1 - y_lo if flip_lo else y_lo) * 8 + z, y_hi * 8 + x * 2 + core)

    moves = [
        (False, y_hi, x + 1 - 2 * (x % 2), (x // 2 + x % 2) % 2),
        (True, y_hi, x, (y_hi + y_lo) % 2),
        (False, y_hi, 3 - x, x // 2),
        (True, 1 - y_hi, x, y_hi),
    ]
    links = [device(*move[:3]) for move in moves]
    bits = [[moves[(c + k) % 4][3] for k in range(4)] for c in range(4)]
    partners = [[links[(c + k) % 4] for k in range(4)] for c in range(4)]
    corners = []
    for c in range(4):
        a, b = moves[(c + 2) % 4], moves[(c + 3) % 4]
        along_x, along_y = (a, b) if c % 2 == 0 else (b, a)
        corners.append(device(True, along_y[1], along_x[2]))
    other = device(False, y_hi, x, 1 - core)
    along_z = [None] + [(y_lo * 8 + (z + d) % 8, gy) for d in range(1, 8)]
    along_gy = [None] + [(gx, (gy + d) % 16) for d in range(1, 16)]

    barrier = pltpu.get_barrier_semaphore()
    peers = along_gy[1:] + along_z[1:] + [links[1], links[3]] + corners
    for peer in peers:
        pl.semaphore_signal(barrier, inc=1, device_id=peer, device_id_type=MESH)

    weights = pltpu.make_async_copy(wp, pbuf, psem)
    weights.start()
    tables = [pltpu.make_async_copy(wt.at[c], wbuf.at[c], wsem.at[c]) for c in range(4)]
    extras = [pltpu.make_async_copy(wextra.at[c], part.at[c], esem.at[c]) for c in range(4)]
    for c in range(4):
        tables[c].start()
        extras[c].start()
    thin_rows = pltpu.make_async_copy(tt, tbuf, tsem)
    thin_rows.start()

    def send(src, dst, s, r, to):
        copy = pltpu.make_async_remote_copy(
            src_ref=src, dst_ref=dst, send_sem=s, recv_sem=r, device_id=to, device_id_type=MESH
        )
        copy.start()
        return copy

    def wide_part(c):
        tables[c].wait()
        if c == 0:
            weights.wait()
        both_parts = split_projection(wbuf[c], pbuf[c])
        rows = wbuf.shape[1]
        chunks = [ids_of(r * 16 - 256) for r in range(rows // 16)]
        extras[c].wait()
        for b in range(wslot.shape[2] // BLOCK):
            columns = []
            for g in range(BLOCK // 128):
                at = b * BLOCK + g * 128
                marks = [mark_of(wslot[c, k : k + 1, at : at + 128]) for k in range(WIDE_SLOTS)]
                columns.append(jnp.concatenate([one_hot(marks, chunk) for chunk in chunks], axis=0))
            hits = jnp.concatenate(columns, axis=1)
            both = jnp.dot(both_parts, hits, preferred_element_type=F32)
            found = (both[:128] + both[128:]).T
            for g in range(BLOCK // 128):
                g_lo, g_z = divmod(b * (BLOCK // 128) + g, 8)
                for g_hi in range(2):
                    for g_x in range(4):
                        place = place_of(c, g_lo, g_z, g_hi, g_x)
                        for g_core in range(2):
                            row = g * 128 + g_hi * 64 + g_x * 16 + g_core * 8
                            spot = (c, g_core, place // 8, place % 8)
                            part[spot] = part[spot] + found[row : row + 8]

    def thin_table(i, _):
        groups = tbuf.shape[2] // 256
        lines = jnp.concatenate([tbuf[i, :, g * 256 : g * 256 + 256] for g in range(groups)], axis=0)
        chunks = [ids_of(r * 16) for r in range(16)]
        total = [textra[i, f * 8 : f * 8 + 8, :] for f in range(4)]
        for pair in range(THIN_SLOTS // 2):
            slots = [tslot[i, pair * 2 + k : pair * 2 + k + 1, :] for k in range(2)]
            columns = []
            for slot in slots:
                mark = mark_of((slot & 255).astype(F32))
                columns.append(jnp.concatenate([one_hot([mark], chunk) for chunk in chunks], axis=0))
            low = jnp.concatenate(columns, axis=1)
            found = jnp.dot(lines, low, preferred_element_type=F32)
            for k in range(2):
                group = jnp.broadcast_to(slots[k] >> 8, (8, 128))
                picked = [jnp.zeros((8, 128), F32)] * 4
                for g in range(groups):
                    same = group == g
                    for f in range(4):
                        row = g * 32 + f * 8
                        piece = found[row : row + 8, k * 128 : k * 128 + 128]
                        picked[f] = jnp.where(same, piece, picked[f])
                total = [a + b for a, b in zip(total, picked)]
        for f in range(4):
            sums[pl.ds(pl.multiple_of(i * 32 + f * 8, 8), 8), :] = total[f]
        return 0

    sends = []
    halves = [None] * 4
    first = [None] * 4

    def step_first(c):
        halves[c].wait_recv()
        sends.append(halves[c])
        go, stay = 1 - bits[c][0], bits[c][0]
        for side in (go, stay):
            half = pl.ds(side * 8, 8)
            part[c, core, half] = part[c, core, half] + r0[c, half]
            if side is go:
                first[c] = send(
                    part.at[c, core, half], r1.at[c], ssem.at[1, c], rsem.at[1, c], partners[c][0]
                )

    for c in range(4):
        wide_part(c)
        if c == 0:
            pl.semaphore_wait(barrier, len(peers))
        halves[c] = send(
            part.at[c, 1 - core], r0.at[c], ssem.at[0, c], rsem.at[0, c], other
        )
        if c > 0:
            step_first(c - 1)
    step_first(3)

    thin_rows.wait()
    lax.fori_loop(0, tbuf.shape[0], thin_table, 0)
    for h in range(2):
        th[h] = sums[h * 128 : h * 128 + 128, :].T.reshape(16, 8, 128)

    second = []
    for c in range(4):
        first[c].wait_recv()
        sends.append(first[c])
        kept, go, stay = bits[c][0], 1 - bits[c][1], bits[c][1]
        for side in (go, stay):
            half = pl.ds(side * 4, 4)
            r1[c, half] = r1[c, half] + part[c, core, pl.ds(kept * 8 + side * 4, 4)]
            if side is go:
                second.append(
                    send(r1.at[c, half], r2.at[c], ssem.at[2, c], rsem.at[2, c], partners[c][1])
                )
    thins = []
    for d in range(1, 16):
        thins.append(send(th.at[:, along_gy[d][1]], rt.at[d], ts.at[d], tr.at[d], along_gy[d]))

    thirds = []
    for c in range(4):
        second[c].wait_recv()
        sends.append(second[c])
        kept, (b2, b3) = bits[c][1], bits[c][2:]
        ways = [
            (1 - b2, 1 - b3, corners[c]),
            (1 - b2, b3, partners[c][2]),
            (b2, 1 - b3, partners[c][3]),
        ]
        row = []
        for j, (i2, i3, to) in enumerate(ways):
            here = i2 * 2 + i3
            r2[c, here] = r2[c, here] + r1[c, kept * 4 + here]
            row.append(send(r2.at[c, here], rm.at[c, j], ms.at[c, j], mr.at[c, j], to))
        thirds.append(row)

    for c in range(4):
        here = bits[c][2] * 2 + bits[c][3]
        total = r2[c, here] + r1[c, bits[c][1] * 4 + here]
        for j in range(3):
            thirds[c][j].wait_recv()
            sends.append(thirds[c][j])
            total = total + rm[c, j]
        r4[c] = total
    lasts = []
    for d in (4, 3, 5, 2, 6, 1, 7):
        lasts.append(
            (d, send(r4.at[:, (z + d) % 8], rz.at[d], zs.at[d], zr.at[d], along_z[d]))
        )

    for copy in thins:
        copy.wait_recv()
    pooled = th[:, gy]
    for d in range(1, 16):
        pooled = pooled + rt[d]
    group = lax.broadcasted_iota(I32, (8, 128), 1) // 32
    for h in range(2):
        rows = jnp.concatenate([jnp.where(group == g, pooled[h], 0.0) for g in range(4)], axis=0)
        projected = jnp.dot(
            rows, pj[h].astype(F32), preferred_element_type=F32, precision=lax.Precision.HIGHEST
        )
        for g in range(4):
            at = 512 + (h * 4 + g) * 128
            out[:, at : at + 128] = projected[g * 8 : g * 8 + 8]

    total = r4[:, z]
    for d, copy in lasts:
        copy.wait_recv()
        total = total + rz[d]
    for c in range(4):
        out[:, c * 128 : c * 128 + 128] = total[c]
    for copy in sends + thins + [copy for _, copy in lasts]:
        copy.wait_send()


def pool(wslot, tslot, wextra, textra, wide_table, wide_proj, thin_table, thin_proj):
    vmem, anywhere = pl.BlockSpec(memory_space=pltpu.VMEM), pl.BlockSpec(memory_space=pl.ANY)
    dma = pltpu.SemaphoreType.DMA
    return pl.pallas_call(
        pool_kernel,
        in_specs=[vmem] * 4 + [anywhere] * 4,
        out_specs=vmem,
        out_shape=jax.ShapeDtypeStruct((8, 1536), F32),
        scratch_shapes=[
            pltpu.VMEM((4, 2, 16, 8, 8, 128), F32),
            pltpu.VMEM(wide_table.shape, BF16),
            pltpu.VMEM(wide_proj.shape, BF16),
            pltpu.VMEM(thin_table.shape, BF16),
            pltpu.VMEM((256, 128), F32),
            pltpu.VMEM((2, 16, 8, 128), F32),
            pltpu.VMEM((4, 16, 8, 8, 128), F32),
            pltpu.VMEM((4, 8, 8, 8, 128), F32),
            pltpu.VMEM((4, 4, 8, 8, 128), F32),
            pltpu.VMEM((4, 3, 8, 8, 128), F32),
            pltpu.VMEM((4, 8, 8, 128), F32),
            pltpu.VMEM((8, 4, 8, 128), F32),
            pltpu.VMEM((16, 2, 8, 128), F32),
            dma((4,)),
            dma((4,)),
            dma,
            dma,
            dma((3, 4)),
            dma((3, 4)),
            dma((4, 3)),
            dma((4, 3)),
            dma((8,)),
            dma((8,)),
            dma((16,)),
            dma((16,)),
        ],
        compiler_params=pltpu.CompilerParams(collective_id=0, has_side_effects=True),
    )(
        wslot, tslot, textra, thin_proj.reshape(2, 128, 128),
        wextra.reshape(4, 2, 16, 8, 8, 128), wide_table, wide_proj, thin_table,
    )


def local(wide_index, wide_table, wide_proj, thin_index, thin_table, thin_proj):
    wslot, tslot, wextra, textra = find(wide_index, thin_index, wide_table, wide_proj, thin_table)
    out = pool(wslot, tslot, wextra, textra, wide_table, wide_proj, thin_table, thin_proj)
    return out[:, :512], out[:, 512:]


def solution(mesh):
    placed = (P(), P(None, GX_GY, None), P(), P(None, None, "gx"), P(None, None, "gy"), P())
    return jax.shard_map(
        local,
        mesh=mesh,
        in_specs=placed,
        out_specs=(P(GX_GY, None), P(GX_GY, None)),
        check_vma=False,
    )
```

```python
import functools

import jax
import jax.numpy as jnp
from jax import lax
from jax.experimental import pallas as pl
from jax.experimental.pallas import tpu as pltpu
from jax.sharding import PartitionSpec as P

F32, BF16, I32 = jnp.float32, jnp.bfloat16, jnp.int32
MESH = pl.DeviceIdType.MESH
GX_GY = ("gx", "gy")

WIDE_SLOTS = 4
THIN_SLOTS = 12
BLOCK = 256


def keys_of(index, first, count, axis):
    row = index - first
    place = lax.broadcasted_iota(I32, row.shape, axis)
    return jnp.where((row >= 0) & (row < count), row * 32 + place, -1)


def next_slot(keys, slot, axis=0):
    return jnp.max(jnp.where(keys < slot, keys, -1), axis=axis, keepdims=True)


def mark_of(values):
    return jnp.broadcast_to(values, (16, values.shape[1])).astype(BF16)


def wide_mark(slot):
    return jnp.where(slot < 0, 256, (slot >> 5) - 256).astype(F32)


def ids_of(first):
    return (lax.broadcasted_iota(I32, (16, 128), 0) + first).astype(F32).astype(BF16)


def one_hot(marks, chunk):
    one, zero = jnp.ones((16, 128), BF16), jnp.zeros((16, 128), BF16)
    hit = jnp.where(chunk == marks[0], one, zero)
    for mark in marks[1:]:
        hit = hit + jnp.where(chunk == mark, one, zero)
    return hit


def split_projection(table, weight):
    projected = jnp.dot(table, weight, preferred_element_type=F32).T
    high = projected.astype(BF16)
    low = (projected - high.astype(F32)).astype(BF16)
    return jnp.concatenate([high, low], axis=0)


def place_of(q, y_lo, y_hi, x):
    bits = ((x // 2) ^ (x % 2), y_hi ^ y_lo, x // 2, y_hi)
    return sum((8 >> ((d - q) % 4)) * bits[d] for d in range(4))


def find_kernel(rows_w, rows_t, wi, ti, wslot, tslot, wmore, tmore, left):
    gx, gy = lax.axis_index("gx"), lax.axis_index("gy")
    tables, _, bags = wi.shape
    first_w, first_t = (gx * 16 + gy) * rows_w, gy * rows_t

    most = jnp.full((1, 128), -1, I32)
    for t in range(tables):
        for b in range(bags // BLOCK):
            at = slice(b * BLOCK, (b + 1) * BLOCK)
            keys = keys_of(wi[t, :, at], first_w, rows_w, 0)
            slot = jnp.max(keys, axis=0, keepdims=True)
            for k in range(WIDE_SLOTS):
                wslot[t, k : k + 1, at] = wide_mark(slot)
                slot = next_slot(keys, slot)
            wmore[t, :, at] = slot
            for c in range(BLOCK // 128):
                most = jnp.maximum(most, slot[:, c * 128 : c * 128 + 128])
    left[0] = jnp.broadcast_to(most, (8, 128))

    thin_keys = keys_of(ti[...], first_t, rows_t, 1)
    slot = jnp.max(thin_keys, axis=1, keepdims=True)
    for k in range(THIN_SLOTS):
        tslot[:, k : k + 1, :] = slot >> 5
        slot = next_slot(thin_keys, slot, 1)
    tmore[...] = slot
    left[1] = jnp.broadcast_to(jnp.max(slot, axis=0), (8, 128))


def spill_kernel(
    wi, ti, wmore, tmore, left, wt, wp, tt, wextra, textra,
    wkeys, hits, proj, lines, low,
):
    gx, gy = lax.axis_index("gx"), lax.axis_index("gy")
    tables, _, bags = wi.shape
    rows_w, rows_t = wt.shape[1], tt.shape[2]
    first_w, first_t = (gx * 16 + gy) * rows_w, gy * rows_t
    blocks = bags // BLOCK
    wextra[...] = jnp.zeros_like(wextra)
    textra[...] = jnp.zeros_like(textra)
    wide_left, thin_left = jnp.max(left[0]), jnp.max(left[1])

    @pl.when(wide_left >= 0)
    def _():
        wkeys[...] = keys_of(wi[...], first_w, rows_w, 1)

        def table(t, _):
            @pl.when(jnp.max(wmore[t]) >= 0)
            def _():
                proj[...] = split_projection(wt[t], wp[t])

                def block(b, _):
                    at = pl.ds(pl.multiple_of(b * BLOCK, BLOCK), BLOCK)
                    top = jnp.max(wmore[t, :, at])

                    @pl.when(top >= 0)
                    def _():
                        hits[...] = jnp.zeros_like(hits)

                        def body(carry):
                            slot, _ = carry
                            for c in range(BLOCK // 128):
                                mark = mark_of(wide_mark(slot[:, c * 128 : c * 128 + 128]))
                                for r in range(rows_w // 16):
                                    spot = (slice(r * 16, r * 16 + 16), slice(c * 128, c * 128 + 128))
                                    hits[spot] = hits[spot] + one_hot([mark], ids_of(r * 16 - 256))
                            slot = next_slot(wkeys[t, :, at], slot)
                            return slot, jnp.max(slot)

                        lax.while_loop(lambda carry: carry[1] >= 0, body, (wmore[t, :, at], top))
                        both = jnp.dot(proj[...], hits[...], preferred_element_type=F32)
                        found = (both[:128] + both[128:]).T
                        for g in range(BLOCK // 128):
                            group = b * (BLOCK // 128) + g
                            y_lo, z = group // 8, group % 8
                            quarter = z // 2
                            step = [8 >> ((d - quarter + 4) % 4) for d in range(4)]
                            for y_hi in range(2):
                                crossed = (y_hi + y_lo) % 2
                                for x in range(4):
                                    place = step[0] * ((x // 2) ^ (x % 2)) + step[1] * crossed
                                    place = place + step[2] * (x // 2) + step[3] * y_hi
                                    place = quarter * 32 + place * 2 + z % 2
                                    for core in range(2):
                                        row = g * 128 + y_hi * 64 + x * 16 + core * 8
                                        wextra[t, core * 128 + place] = found[row : row + 8]

                    return 0

                lax.fori_loop(0, blocks, block, 0)

            return 0

        lax.fori_loop(0, tables, table, 0)

    @pl.when(thin_left >= 0)
    def _():
        groups = rows_t // 256

        def table(i, _):
            keys = keys_of(ti[i], first_t, rows_t, 0)
            slot = tmore[i]
            top = jnp.max(slot)

            @pl.when(top >= 0)
            def _():
                for g in range(groups):
                    lines[g * 32 : g * 32 + 32, :] = tt[i, :, g * 256 : g * 256 + 256]

                def body(carry):
                    slot, _ = carry
                    mark = mark_of(((slot >> 5) & 255).astype(F32))
                    for r in range(16):
                        low[r * 16 : r * 16 + 16, :] = one_hot([mark], ids_of(r * 16))
                    found = jnp.dot(lines[...], low[...], preferred_element_type=F32)
                    group = jnp.broadcast_to(slot >> 13, (32, 128))
                    total = textra[i]
                    for g in range(groups):
                        total = total + jnp.where(group == g, found[g * 32 : g * 32 + 32], 0.0)
                    textra[i] = total
                    slot = next_slot(keys, slot)
                    return slot, jnp.max(slot)

                lax.while_loop(lambda carry: carry[1] >= 0, body, (slot, top))

            return 0

        lax.fori_loop(0, ti.shape[0], table, 0)


def find(wide_index, thin_index, wide_table, wide_proj, thin_table):
    tw, _, bags = wide_index.shape
    tt, _, own_bags = thin_index.shape
    rows_w = wide_table.shape[1]
    wt, rows_t = thin_table.shape[1:]
    vmem = pl.BlockSpec(memory_space=pltpu.VMEM)
    params = pltpu.CompilerParams(vmem_limit_bytes=16 * 2**20)
    wslot, tslot, wmore, tmore, left = pl.pallas_call(
        functools.partial(find_kernel, rows_w, rows_t),
        in_specs=[vmem] * 2,
        out_specs=[vmem] * 5,
        out_shape=[
            jax.ShapeDtypeStruct((tw, WIDE_SLOTS, bags), F32),
            jax.ShapeDtypeStruct((tt, THIN_SLOTS, own_bags), I32),
            jax.ShapeDtypeStruct((tw, 1, bags), I32),
            jax.ShapeDtypeStruct((tt, 1, own_bags), I32),
            jax.ShapeDtypeStruct((2, 8, 128), I32),
        ],
        compiler_params=params,
        cost_estimate=pl.CostEstimate(flops=4 * 10**9, bytes_accessed=1 << 20, transcendentals=0),
    )(wide_index, thin_index)
    wextra, textra = pl.pallas_call(
        spill_kernel,
        in_specs=[vmem] * 8,
        out_specs=[vmem] * 2,
        out_shape=[
            jax.ShapeDtypeStruct((tw, bags // 8, 8, 128), F32),
            jax.ShapeDtypeStruct((tt, wt, own_bags), F32),
        ],
        scratch_shapes=[
            pltpu.VMEM(wide_index.shape, I32),
            pltpu.VMEM((rows_w, BLOCK), BF16),
            pltpu.VMEM((256, rows_w), BF16),
            pltpu.VMEM((rows_t // 256 * wt, 256), BF16),
            pltpu.VMEM((256, 128), BF16),
        ],
        compiler_params=params,
    )(wide_index, thin_index, wmore, tmore, left, wide_table, wide_proj, thin_table)
    return wslot, tslot, wextra, textra


def pool_kernel(
    wslot, tslot, wextra, textra, wt, wp, tt, pj, out,
    part, sums, th, r0, r1, r2, rm, r4, rz, rt,
    hs, hr, ss, sr, ms, mr, zs, zr, ts, tr,
):
    gx, gy = lax.axis_index("gx"), lax.axis_index("gy")
    y_lo, z = gx // 8, gx % 8
    y_hi, x, core = gy // 8, (gy // 2) % 4, gy % 2
    every = range(4)

    def device(flip_lo, y_hi, x, core=core):
        return ((1 - y_lo if flip_lo else y_lo) * 8 + z, y_hi * 8 + x * 2 + core)

    moves = [
        (False, y_hi, x + 1 - 2 * (x % 2), (x // 2 + x % 2) % 2),
        (True, y_hi, x, (y_hi + y_lo) % 2),
        (False, y_hi, 3 - x, x // 2),
        (True, 1 - y_hi, x, y_hi),
    ]
    links = [device(*move[:3]) for move in moves]
    bits = [[moves[(q + k) % 4][3] for k in every] for q in every]
    partners = [[links[(q + k) % 4] for k in every] for q in every]
    corners = []
    for q in every:
        a, b = moves[(q + 2) % 4], moves[(q + 3) % 4]
        along_x, along_y = (a, b) if q % 2 == 0 else (b, a)
        corners.append(device(True, along_y[1], along_x[2]))
    other = device(False, y_hi, x, 1 - core)
    along_z = [None] + [(y_lo * 8 + (z + d) % 8, gy) for d in range(1, 8)]
    along_gy = [None] + [(gx, (gy + d) % 16) for d in range(1, 16)]

    barrier = pltpu.get_barrier_semaphore()
    peers = along_gy[1:] + along_z[1:] + [links[1], links[3]] + corners
    for peer in peers:
        pl.semaphore_signal(barrier, inc=1, device_id=peer, device_id_type=MESH)

    sends = []

    def send(src, dst, s, r, to):
        copy = pltpu.make_async_remote_copy(
            src_ref=src, dst_ref=dst, send_sem=s, recv_sem=r, device_id=to, device_id_type=MESH
        )
        copy.start()
        sends.append(copy)
        return copy

    def wide_part(c):
        both_parts = split_projection(wt[c], wp[c])
        chunks = [ids_of(r * 16 - 256) for r in range(wt.shape[1] // 16)]
        for b in range(wslot.shape[2] // BLOCK):
            columns = []
            for g in range(BLOCK // 128):
                at = b * BLOCK + g * 128
                marks = [mark_of(wslot[c, k : k + 1, at : at + 128]) for k in range(WIDE_SLOTS)]
                columns.append(jnp.concatenate([one_hot(marks, chunk) for chunk in chunks], axis=0))
            hits = jnp.concatenate(columns, axis=1)
            both = jnp.dot(both_parts, hits, preferred_element_type=F32)
            found = (both[:128] + both[128:]).T
            for g in range(BLOCK // 128):
                g_lo, g_z = divmod(b * (BLOCK // 128) + g, 8)
                for g_hi in range(2):
                    for g_x in every:
                        place = place_of(g_z // 2, g_lo, g_hi, g_x)
                        for g_core in range(2):
                            row = g * 128 + g_hi * 64 + g_x * 16 + g_core * 8
                            spot = (c, g_core, g_z // 2, place, g_z % 2)
                            part[spot] = wextra[spot] + found[row : row + 8]

    def thin_table(i, _):
        groups = tt.shape[2] // 256
        lines = jnp.concatenate([tt[i, :, g * 256 : g * 256 + 256] for g in range(groups)], axis=0)
        chunks = [ids_of(r * 16) for r in range(16)]
        total = [textra[i, f * 8 : f * 8 + 8, :] for f in every]
        for pair in range(THIN_SLOTS // 2):
            slots = [tslot[i, pair * 2 + k : pair * 2 + k + 1, :] for k in range(2)]
            columns = []
            for slot in slots:
                mark = mark_of((slot & 255).astype(F32))
                columns.append(jnp.concatenate([one_hot([mark], chunk) for chunk in chunks], axis=0))
            low = jnp.concatenate(columns, axis=1)
            found = jnp.dot(lines, low, preferred_element_type=F32)
            for k in range(2):
                group = jnp.broadcast_to(slots[k] >> 8, (8, 128))
                picked = [jnp.zeros((8, 128), F32)] * 4
                for g in range(groups):
                    same = group == g
                    for f in every:
                        row = g * 32 + f * 8
                        piece = found[row : row + 8, k * 128 : k * 128 + 128]
                        picked[f] = jnp.where(same, piece, picked[f])
                total = [a + b for a, b in zip(total, picked)]
        for f in every:
            sums[pl.ds(pl.multiple_of(i * 32 + f * 8, 8), 8), :] = total[f]
        return 0

    halves, first, second, third, lasts = {}, {}, {}, {}, {}

    def send_half(c):
        halves[c] = send(part.at[c, 1 - core], r0.at[c], hs.at[c], hr.at[c], other)

    def send_first(c):
        halves[c].wait_recv()
        for turn in range(2):
            for q in every:
                half = pl.ds((1 - bits[q][0] if turn == 0 else bits[q][0]) * 8, 8)
                part[c, core, q, half] = part[c, core, q, half] + r0[c, q, half]
                if turn == 0:
                    first[c, q] = send(
                        part.at[c, core, q, half], r1.at[c, q], ss.at[0, c, q], sr.at[0, c, q],
                        partners[q][0],
                    )

    def send_second(c):
        for q in every:
            first[c, q].wait_recv()
            side = 1 - bits[q][1]
            half = pl.ds(side * 4, 4)
            r1[c, q, half] = r1[c, q, half] + part[c, core, q, pl.ds(bits[q][0] * 8 + side * 4, 4)]
            second[c, q] = send(
                r1.at[c, q, half], r2.at[c, q], ss.at[1, c, q], sr.at[1, c, q], partners[q][1]
            )
        for q in every:
            side = bits[q][1]
            half = pl.ds(side * 4, 4)
            r1[c, q, half] = r1[c, q, half] + part[c, core, q, pl.ds(bits[q][0] * 8 + side * 4, 4)]

    def send_third(c):
        for q in every:
            second[c, q].wait_recv()
            b1, b2, b3 = bits[q][1:]
            ways = [
                (1 - b2, 1 - b3, corners[q]),
                (1 - b2, b3, partners[q][2]),
                (b2, 1 - b3, partners[q][3]),
            ]
            for j, (i2, i3, to) in enumerate(ways):
                here = i2 * 2 + i3
                r2[c, q, here] = r2[c, q, here] + r1[c, q, b1 * 4 + here]
                third[c, q, j] = send(
                    r2.at[c, q, here], rm.at[c, q, j], ms.at[c, q, j], mr.at[c, q, j], to
                )

    def send_last(c):
        for q in every:
            b1, b2, b3 = bits[q][1:]
            here = b2 * 2 + b3
            total = r2[c, q, here] + r1[c, q, b1 * 4 + here]
            for j in (1, 2, 0):
                third[c, q, j].wait_recv()
                total = total + rm[c, q, j]
            r4[c, q * 2 : q * 2 + 2] = total
        for d in (4, 3, 5, 2, 6, 1, 7):
            lasts[c, d] = send(
                r4.at[c, (z + d) % 8], rz.at[d, c], zs.at[d, c], zr.at[d, c], along_z[d]
            )

    def thin_tables(begin, end):
        lax.fori_loop(begin, end, thin_table, 0)

    wide_part(0)
    pl.semaphore_wait(barrier, len(peers))
    send_half(0)
    wide_part(1)
    send_half(1)
    wide_part(2)
    send_half(2)
    send_first(0)
    wide_part(3)
    send_half(3)
    send_first(1)
    thin_tables(0, 2)
    send_first(2)
    send_second(0)
    thin_tables(2, 4)
    send_first(3)
    send_second(1)
    thin_tables(4, 6)
    send_second(2)
    send_third(0)
    thin_tables(6, 8)
    for h in range(2):
        th[h] = sums[h * 128 : h * 128 + 128, :].T.reshape(16, 8, 128)
    thins = []
    for d in range(1, 16):
        thins.append(send(th.at[:, along_gy[d][1]], rt.at[d], ts.at[d], tr.at[d], along_gy[d]))
    send_second(3)
    send_third(1)
    send_last(0)
    send_third(2)
    send_last(1)
    send_third(3)
    send_last(2)

    for copy in thins:
        copy.wait_recv()
    pooled = th[:, gy]
    for d in range(1, 16):
        pooled = pooled + rt[d]
    group = lax.broadcasted_iota(I32, (8, 128), 1) // 32
    for h in range(2):
        rows = jnp.concatenate([jnp.where(group == g, pooled[h], 0.0) for g in every], axis=0)
        projected = jnp.dot(
            rows, pj[h].astype(F32), preferred_element_type=F32, precision=lax.Precision.HIGHEST
        )
        for g in every:
            at = 512 + (h * 4 + g) * 128
            out[:, at : at + 128] = projected[g * 8 : g * 8 + 8]

    send_last(3)
    for c in every:
        total = r4[c, z]
        for d in (1, 7, 2, 6, 3, 5, 4):
            lasts[c, d].wait_recv()
            total = total + rz[d, c]
        out[:, c * 128 : c * 128 + 128] = total
    for copy in sends:
        copy.wait_send()


def pool(wslot, tslot, wextra, textra, wide_table, wide_proj, thin_table, thin_proj):
    vmem = pl.BlockSpec(memory_space=pltpu.VMEM)
    dma = pltpu.SemaphoreType.DMA
    return pl.pallas_call(
        pool_kernel,
        in_specs=[vmem] * 8,
        out_specs=vmem,
        out_shape=jax.ShapeDtypeStruct((8, 1536), F32),
        scratch_shapes=[
            pltpu.VMEM((4, 2, 4, 16, 2, 8, 128), F32),
            pltpu.VMEM((256, 128), F32),
            pltpu.VMEM((2, 16, 8, 128), F32),
            pltpu.VMEM((4, 4, 16, 2, 8, 128), F32),
            pltpu.VMEM((4, 4, 8, 2, 8, 128), F32),
            pltpu.VMEM((4, 4, 4, 2, 8, 128), F32),
            pltpu.VMEM((4, 4, 3, 2, 8, 128), F32),
            pltpu.VMEM((4, 8, 8, 128), F32),
            pltpu.VMEM((8, 4, 8, 128), F32),
            pltpu.VMEM((16, 2, 8, 128), F32),
            dma((4,)),
            dma((4,)),
            dma((2, 4, 4)),
            dma((2, 4, 4)),
            dma((4, 4, 3)),
            dma((4, 4, 3)),
            dma((8, 4)),
            dma((8, 4)),
            dma((16,)),
            dma((16,)),
        ],
        compiler_params=pltpu.CompilerParams(
            collective_id=0, has_side_effects=True, vmem_limit_bytes=24 * 2**20
        ),
    )(
        wslot, tslot, wextra.reshape(4, 2, 4, 16, 2, 8, 128), textra,
        wide_table, wide_proj, thin_table, thin_proj.reshape(2, 128, 128),
    )


def local(wide_index, wide_table, wide_proj, thin_index, thin_table, thin_proj):
    wslot, tslot, wextra, textra = find(wide_index, thin_index, wide_table, wide_proj, thin_table)
    out = pool(wslot, tslot, wextra, textra, wide_table, wide_proj, thin_table, thin_proj)
    return out[:, :512], out[:, 512:]


def solution(mesh):
    placed = (P(), P(None, GX_GY, None), P(), P(None, None, "gx"), P(None, None, "gy"), P())
    return jax.shard_map(
        local,
        mesh=mesh,
        in_specs=placed,
        out_specs=(P(GX_GY, None), P(GX_GY, None)),
        check_vma=False,
    )
```

```python
import functools

import jax
import jax.numpy as jnp
from jax import lax
from jax.experimental import pallas as pl
from jax.experimental.pallas import tpu as pltpu
from jax.sharding import PartitionSpec as P

F32, BF16, I32 = jnp.float32, jnp.bfloat16, jnp.int32
MESH = pl.DeviceIdType.MESH
GX_GY = ("gx", "gy")

WIDE_SLOTS = 4
THIN_SLOTS = 12
BLOCK = 256


def keys_of(index, first, count, axis):
    row = index - first
    place = lax.broadcasted_iota(I32, row.shape, axis)
    return jnp.where((row >= 0) & (row < count), row * 32 + place, -1)


def next_slot(keys, slot, axis=0):
    return jnp.max(jnp.where(keys < slot, keys, -1), axis=axis, keepdims=True)


def mark_of(values):
    return jnp.broadcast_to(values, (16, values.shape[1])).astype(BF16)


def wide_mark(slot):
    return jnp.where(slot < 0, 256, (slot >> 5) - 256).astype(F32)


def ids_of(first):
    return (lax.broadcasted_iota(I32, (16, 128), 0) + first).astype(F32).astype(BF16)


def one_hot(marks, chunk):
    one, zero = jnp.ones((16, 128), BF16), jnp.zeros((16, 128), BF16)
    hit = jnp.where(chunk == marks[0], one, zero)
    for mark in marks[1:]:
        hit = hit + jnp.where(chunk == mark, one, zero)
    return hit


def split_projection(table, weight):
    projected = jnp.dot(table, weight, preferred_element_type=F32).T
    high = projected.astype(BF16)
    low = (projected - high.astype(F32)).astype(BF16)
    return jnp.concatenate([high, low], axis=0)


def place_of(q, y_lo, y_hi, x):
    bits = ((x // 2) ^ (x % 2), y_hi ^ y_lo, x // 2, y_hi)
    return sum((8 >> ((d - q) % 4)) * bits[d] for d in range(4))


def find_kernel(rows_w, rows_t, wi, ti, wslot, tslot, wmore, tmore, left):
    gx, gy = lax.axis_index("gx"), lax.axis_index("gy")
    tables, _, bags = wi.shape
    first_w, first_t = (gx * 16 + gy) * rows_w, gy * rows_t

    most = jnp.full((1, 128), -1, I32)
    for t in range(tables):
        for b in range(bags // BLOCK):
            at = slice(b * BLOCK, (b + 1) * BLOCK)
            keys = keys_of(wi[t, :, at], first_w, rows_w, 0)
            slot = jnp.max(keys, axis=0, keepdims=True)
            for k in range(WIDE_SLOTS):
                wslot[t, k : k + 1, at] = wide_mark(slot)
                slot = next_slot(keys, slot)
            wmore[t, :, at] = slot
            for c in range(BLOCK // 128):
                most = jnp.maximum(most, slot[:, c * 128 : c * 128 + 128])
    left[0] = jnp.broadcast_to(most, (8, 128))

    thin_keys = keys_of(ti[...], first_t, rows_t, 1)
    slot = jnp.max(thin_keys, axis=1, keepdims=True)
    for k in range(THIN_SLOTS):
        tslot[:, k : k + 1, :] = slot >> 5
        slot = next_slot(thin_keys, slot, 1)
    tmore[...] = slot
    left[1] = jnp.broadcast_to(jnp.max(slot, axis=0), (8, 128))


def spill_kernel(
    wi, ti, wmore, tmore, left, wt, wp, tt, wextra, textra,
    wkeys, hits, proj, lines, low,
):
    gx, gy = lax.axis_index("gx"), lax.axis_index("gy")
    tables, _, bags = wi.shape
    rows_w, rows_t = wt.shape[1], tt.shape[2]
    first_w, first_t = (gx * 16 + gy) * rows_w, gy * rows_t
    blocks = bags // BLOCK
    wextra[...] = jnp.zeros_like(wextra)
    textra[...] = jnp.zeros_like(textra)
    wide_left, thin_left = jnp.max(left[0]), jnp.max(left[1])

    @pl.when(wide_left >= 0)
    def _():
        wkeys[...] = keys_of(wi[...], first_w, rows_w, 1)

        def table(t, _):
            @pl.when(jnp.max(wmore[t]) >= 0)
            def _():
                proj[...] = split_projection(wt[t], wp[t])

                def block(b, _):
                    at = pl.ds(pl.multiple_of(b * BLOCK, BLOCK), BLOCK)
                    top = jnp.max(wmore[t, :, at])

                    @pl.when(top >= 0)
                    def _():
                        hits[...] = jnp.zeros_like(hits)

                        def body(carry):
                            slot, _ = carry
                            for c in range(BLOCK // 128):
                                mark = mark_of(wide_mark(slot[:, c * 128 : c * 128 + 128]))
                                for r in range(rows_w // 16):
                                    spot = (slice(r * 16, r * 16 + 16), slice(c * 128, c * 128 + 128))
                                    hits[spot] = hits[spot] + one_hot([mark], ids_of(r * 16 - 256))
                            slot = next_slot(wkeys[t, :, at], slot)
                            return slot, jnp.max(slot)

                        lax.while_loop(lambda carry: carry[1] >= 0, body, (wmore[t, :, at], top))
                        both = jnp.dot(proj[...], hits[...], preferred_element_type=F32)
                        found = (both[:128] + both[128:]).T
                        for g in range(BLOCK // 128):
                            group = b * (BLOCK // 128) + g
                            y_lo, z = group // 8, group % 8
                            quarter = z // 2
                            step = [8 >> ((d - quarter + 4) % 4) for d in range(4)]
                            for y_hi in range(2):
                                crossed = (y_hi + y_lo) % 2
                                for x in range(4):
                                    place = step[0] * ((x // 2) ^ (x % 2)) + step[1] * crossed
                                    place = place + step[2] * (x // 2) + step[3] * y_hi
                                    place = quarter * 32 + place * 2 + z % 2
                                    for core in range(2):
                                        row = g * 128 + y_hi * 64 + x * 16 + core * 8
                                        wextra[t, core * 128 + place] = found[row : row + 8]

                    return 0

                lax.fori_loop(0, blocks, block, 0)

            return 0

        lax.fori_loop(0, tables, table, 0)

    @pl.when(thin_left >= 0)
    def _():
        groups = rows_t // 256

        def table(i, _):
            keys = keys_of(ti[i], first_t, rows_t, 0)
            slot = tmore[i]
            top = jnp.max(slot)

            @pl.when(top >= 0)
            def _():
                for g in range(groups):
                    lines[g * 32 : g * 32 + 32, :] = tt[i, :, g * 256 : g * 256 + 256]

                def body(carry):
                    slot, _ = carry
                    mark = mark_of(((slot >> 5) & 255).astype(F32))
                    for r in range(16):
                        low[r * 16 : r * 16 + 16, :] = one_hot([mark], ids_of(r * 16))
                    found = jnp.dot(lines[...], low[...], preferred_element_type=F32)
                    group = jnp.broadcast_to(slot >> 13, (32, 128))
                    total = textra[i]
                    for g in range(groups):
                        total = total + jnp.where(group == g, found[g * 32 : g * 32 + 32], 0.0)
                    textra[i] = total
                    slot = next_slot(keys, slot)
                    return slot, jnp.max(slot)

                lax.while_loop(lambda carry: carry[1] >= 0, body, (slot, top))

            return 0

        lax.fori_loop(0, ti.shape[0], table, 0)


def find(wide_index, thin_index, wide_table, wide_proj, thin_table):
    tw, _, bags = wide_index.shape
    tt, _, own_bags = thin_index.shape
    rows_w = wide_table.shape[1]
    wt, rows_t = thin_table.shape[1:]
    vmem = pl.BlockSpec(memory_space=pltpu.VMEM)
    params = pltpu.CompilerParams(vmem_limit_bytes=16 * 2**20)
    wslot, tslot, wmore, tmore, left = pl.pallas_call(
        functools.partial(find_kernel, rows_w, rows_t),
        in_specs=[vmem] * 2,
        out_specs=[vmem] * 5,
        out_shape=[
            jax.ShapeDtypeStruct((tw, WIDE_SLOTS, bags), F32),
            jax.ShapeDtypeStruct((tt, THIN_SLOTS, own_bags), I32),
            jax.ShapeDtypeStruct((tw, 1, bags), I32),
            jax.ShapeDtypeStruct((tt, 1, own_bags), I32),
            jax.ShapeDtypeStruct((2, 8, 128), I32),
        ],
        compiler_params=params,
        cost_estimate=pl.CostEstimate(flops=4 * 10**9, bytes_accessed=1 << 20, transcendentals=0),
    )(wide_index, thin_index)
    wextra, textra = pl.pallas_call(
        spill_kernel,
        in_specs=[vmem] * 8,
        out_specs=[vmem] * 2,
        out_shape=[
            jax.ShapeDtypeStruct((tw, bags // 8, 8, 128), F32),
            jax.ShapeDtypeStruct((tt, wt, own_bags), F32),
        ],
        scratch_shapes=[
            pltpu.VMEM(wide_index.shape, I32),
            pltpu.VMEM((rows_w, BLOCK), BF16),
            pltpu.VMEM((256, rows_w), BF16),
            pltpu.VMEM((rows_t // 256 * wt, 256), BF16),
            pltpu.VMEM((256, 128), BF16),
        ],
        compiler_params=params,
    )(wide_index, thin_index, wmore, tmore, left, wide_table, wide_proj, thin_table)
    return wslot, tslot, wextra, textra


def pool_kernel(
    wslot, tslot, wextra, textra, wt, wp, tt, pj, out,
    part, sums, th, r0, r1, r2, rm, r4, rz, rt,
    hs, hr, ss, sr, ms, mr, zs, zr, ts, tr, entered,
):
    gx, gy = lax.axis_index("gx"), lax.axis_index("gy")
    y_lo, z = gx // 8, gx % 8
    y_hi, x, core = gy // 8, (gy // 2) % 4, gy % 2
    every = range(4)

    def device(flip_lo, y_hi, x, core=core):
        return ((1 - y_lo if flip_lo else y_lo) * 8 + z, y_hi * 8 + x * 2 + core)

    moves = [
        (False, y_hi, x + 1 - 2 * (x % 2), (x // 2 + x % 2) % 2),
        (True, y_hi, x, (y_hi + y_lo) % 2),
        (False, y_hi, 3 - x, x // 2),
        (True, 1 - y_hi, x, y_hi),
    ]
    links = [device(*move[:3]) for move in moves]
    bits = [[moves[(q + k) % 4][3] for k in every] for q in every]
    partners = [[links[(q + k) % 4] for k in every] for q in every]
    corners = []
    for q in every:
        a, b = moves[(q + 2) % 4], moves[(q + 3) % 4]
        along_x, along_y = (a, b) if q % 2 == 0 else (b, a)
        corners.append(device(True, along_y[1], along_x[2]))
    other = device(False, y_hi, x, 1 - core)
    along_z = [None] + [(y_lo * 8 + (z + d) % 8, gy) for d in range(1, 8)]
    along_gy = [None] + [(gx, (gy + d) % 16) for d in range(1, 16)]

    barrier = pltpu.get_barrier_semaphore()
    peers = [other] + links + [along_z[1], along_z[7]]
    for peer in peers:
        pl.semaphore_signal(barrier, inc=1, device_id=peer, device_id_type=MESH)

    def relay(turn):
        if turn > 0:
            pl.semaphore_wait(entered.at[turn - 1], 2)
        if turn < 3:
            for peer in (along_z[1], along_z[7]):
                pl.semaphore_signal(entered.at[turn], inc=1, device_id=peer, device_id_type=MESH)

    sends = []

    def send(src, dst, s, r, to):
        copy = pltpu.make_async_remote_copy(
            src_ref=src, dst_ref=dst, send_sem=s, recv_sem=r, device_id=to, device_id_type=MESH
        )
        copy.start()
        sends.append(copy)
        return copy

    def wide_part(c):
        both_parts = split_projection(wt[c], wp[c])
        chunks = [ids_of(r * 16 - 256) for r in range(wt.shape[1] // 16)]
        for b in range(wslot.shape[2] // BLOCK):
            columns = []
            for g in range(BLOCK // 128):
                at = b * BLOCK + g * 128
                marks = [mark_of(wslot[c, k : k + 1, at : at + 128]) for k in range(WIDE_SLOTS)]
                columns.append(jnp.concatenate([one_hot(marks, chunk) for chunk in chunks], axis=0))
            hits = jnp.concatenate(columns, axis=1)
            both = jnp.dot(both_parts, hits, preferred_element_type=F32)
            found = (both[:128] + both[128:]).T
            for g in range(BLOCK // 128):
                g_lo, g_z = divmod(b * (BLOCK // 128) + g, 8)
                for g_hi in range(2):
                    for g_x in every:
                        place = place_of(g_z // 2, g_lo, g_hi, g_x)
                        for g_core in range(2):
                            row = g * 128 + g_hi * 64 + g_x * 16 + g_core * 8
                            spot = (c, g_core, g_z // 2, place, g_z % 2)
                            part[spot] = wextra[spot] + found[row : row + 8]

    def thin_table(i, _):
        groups = tt.shape[2] // 256
        lines = jnp.concatenate([tt[i, :, g * 256 : g * 256 + 256] for g in range(groups)], axis=0)
        chunks = [ids_of(r * 16) for r in range(16)]
        total = [textra[i, f * 8 : f * 8 + 8, :] for f in every]
        for pair in range(THIN_SLOTS // 2):
            slots = [tslot[i, pair * 2 + k : pair * 2 + k + 1, :] for k in range(2)]
            columns = []
            for slot in slots:
                mark = mark_of((slot & 255).astype(F32))
                columns.append(jnp.concatenate([one_hot([mark], chunk) for chunk in chunks], axis=0))
            low = jnp.concatenate(columns, axis=1)
            found = jnp.dot(lines, low, preferred_element_type=F32)
            for k in range(2):
                group = jnp.broadcast_to(slots[k] >> 8, (8, 128))
                picked = [jnp.zeros((8, 128), F32)] * 4
                for g in range(groups):
                    same = group == g
                    for f in every:
                        row = g * 32 + f * 8
                        piece = found[row : row + 8, k * 128 : k * 128 + 128]
                        picked[f] = jnp.where(same, piece, picked[f])
                total = [a + b for a, b in zip(total, picked)]
        for f in every:
            sums[pl.ds(pl.multiple_of(i * 32 + f * 8, 8), 8), :] = total[f]
        return 0

    halves, first, second, third, lasts = {}, {}, {}, {}, {}

    def send_half(c):
        halves[c] = send(part.at[c, 1 - core], r0.at[c], hs.at[c], hr.at[c], other)

    def send_first(c):
        halves[c].wait_recv()
        for turn in range(2):
            for q in every:
                half = pl.ds((1 - bits[q][0] if turn == 0 else bits[q][0]) * 8, 8)
                part[c, core, q, half] = part[c, core, q, half] + r0[c, q, half]
                if turn == 0:
                    first[c, q] = send(
                        part.at[c, core, q, half], r1.at[c, q], ss.at[0, c, q], sr.at[0, c, q],
                        partners[q][0],
                    )

    def send_second(c):
        for q in every:
            first[c, q].wait_recv()
            side = 1 - bits[q][1]
            half = pl.ds(side * 4, 4)
            r1[c, q, half] = r1[c, q, half] + part[c, core, q, pl.ds(bits[q][0] * 8 + side * 4, 4)]
            second[c, q] = send(
                r1.at[c, q, half], r2.at[c, q], ss.at[1, c, q], sr.at[1, c, q], partners[q][1]
            )
        for q in every:
            side = bits[q][1]
            half = pl.ds(side * 4, 4)
            r1[c, q, half] = r1[c, q, half] + part[c, core, q, pl.ds(bits[q][0] * 8 + side * 4, 4)]

    def send_third(c):
        for q in every:
            second[c, q].wait_recv()
            b1, b2, b3 = bits[q][1:]
            ways = [
                (1 - b2, 1 - b3, corners[q]),
                (1 - b2, b3, partners[q][2]),
                (b2, 1 - b3, partners[q][3]),
            ]
            for j, (i2, i3, to) in enumerate(ways):
                here = i2 * 2 + i3
                r2[c, q, here] = r2[c, q, here] + r1[c, q, b1 * 4 + here]
                third[c, q, j] = send(
                    r2.at[c, q, here], rm.at[c, q, j], ms.at[c, q, j], mr.at[c, q, j], to
                )

    def send_last(c):
        for q in every:
            b1, b2, b3 = bits[q][1:]
            here = b2 * 2 + b3
            total = r2[c, q, here] + r1[c, q, b1 * 4 + here]
            for j in (1, 2, 0):
                third[c, q, j].wait_recv()
                total = total + rm[c, q, j]
            r4[c, q * 2 : q * 2 + 2] = total
        for d in (4, 3, 5, 2, 6, 1, 7):
            lasts[c, d] = send(
                r4.at[c, (z + d) % 8], rz.at[d, c], zs.at[d, c], zr.at[d, c], along_z[d]
            )

    def thin_tables(begin, end):
        lax.fori_loop(begin, end, thin_table, 0)

    wide_part(0)
    pl.semaphore_wait(barrier, len(peers))
    send_half(0)
    relay(0)
    wide_part(1)
    send_half(1)
    send_first(0)
    wide_part(2)
    send_half(2)
    send_first(1)
    wide_part(3)
    send_half(3)
    relay(1)
    send_first(2)
    thin_tables(0, 1)
    send_second(0)
    send_first(3)
    relay(2)
    thin_tables(1, 2)
    send_second(1)
    thin_tables(2, 3)
    send_third(0)
    send_second(2)
    relay(3)
    thin_tables(3, 4)
    send_third(1)
    send_second(3)
    thin_tables(4, 6)
    send_last(0)
    send_third(2)
    thin_tables(6, 8)
    for h in range(2):
        th[h] = sums[h * 128 : h * 128 + 128, :].T.reshape(16, 8, 128)
    thins = []
    for d in range(1, 16):
        thins.append(send(th.at[:, along_gy[d][1]], rt.at[d], ts.at[d], tr.at[d], along_gy[d]))
    send_last(1)
    send_third(3)
    send_last(2)

    for copy in thins:
        copy.wait_recv()
    pooled = th[:, gy]
    for d in range(1, 16):
        pooled = pooled + rt[d]
    group = lax.broadcasted_iota(I32, (8, 128), 1) // 32
    for h in range(2):
        rows = jnp.concatenate([jnp.where(group == g, pooled[h], 0.0) for g in every], axis=0)
        projected = jnp.dot(
            rows, pj[h].astype(F32), preferred_element_type=F32, precision=lax.Precision.HIGHEST
        )
        for g in every:
            at = 512 + (h * 4 + g) * 128
            out[:, at : at + 128] = projected[g * 8 : g * 8 + 8]

    send_last(3)
    for c in every:
        total = r4[c, z]
        for d in (1, 7, 2, 6, 3, 5, 4):
            lasts[c, d].wait_recv()
            total = total + rz[d, c]
        out[:, c * 128 : c * 128 + 128] = total
    for copy in sends:
        copy.wait_send()


def pool(wslot, tslot, wextra, textra, wide_table, wide_proj, thin_table, thin_proj):
    vmem = pl.BlockSpec(memory_space=pltpu.VMEM)
    dma = pltpu.SemaphoreType.DMA
    return pl.pallas_call(
        pool_kernel,
        in_specs=[vmem] * 8,
        out_specs=vmem,
        out_shape=jax.ShapeDtypeStruct((8, 1536), F32),
        scratch_shapes=[
            pltpu.VMEM((4, 2, 4, 16, 2, 8, 128), F32),
            pltpu.VMEM((256, 128), F32),
            pltpu.VMEM((2, 16, 8, 128), F32),
            pltpu.VMEM((4, 4, 16, 2, 8, 128), F32),
            pltpu.VMEM((4, 4, 8, 2, 8, 128), F32),
            pltpu.VMEM((4, 4, 4, 2, 8, 128), F32),
            pltpu.VMEM((4, 4, 3, 2, 8, 128), F32),
            pltpu.VMEM((4, 8, 8, 128), F32),
            pltpu.VMEM((8, 4, 8, 128), F32),
            pltpu.VMEM((16, 2, 8, 128), F32),
            dma((4,)),
            dma((4,)),
            dma((2, 4, 4)),
            dma((2, 4, 4)),
            dma((4, 4, 3)),
            dma((4, 4, 3)),
            dma((8, 4)),
            dma((8, 4)),
            dma((16,)),
            dma((16,)),
            pltpu.SemaphoreType.REGULAR((3,)),
        ],
        compiler_params=pltpu.CompilerParams(
            collective_id=0, has_side_effects=True, vmem_limit_bytes=24 * 2**20
        ),
    )(
        wslot, tslot, wextra.reshape(4, 2, 4, 16, 2, 8, 128), textra,
        wide_table, wide_proj, thin_table, thin_proj.reshape(2, 128, 128),
    )


def local(wide_index, wide_table, wide_proj, thin_index, thin_table, thin_proj):
    wslot, tslot, wextra, textra = find(wide_index, thin_index, wide_table, wide_proj, thin_table)
    out = pool(wslot, tslot, wextra, textra, wide_table, wide_proj, thin_table, thin_proj)
    return out[:, :512], out[:, 512:]


def solution(mesh):
    placed = (P(), P(None, GX_GY, None), P(), P(None, None, "gx"), P(None, None, "gy"), P())
    return jax.shard_map(
        local,
        mesh=mesh,
        in_specs=placed,
        out_specs=(P(GX_GY, None), P(GX_GY, None)),
        check_vma=False,
    )
```

```python
import functools

import jax
import jax.numpy as jnp
from jax import lax
from jax.experimental import pallas as pl
from jax.experimental.pallas import tpu as pltpu
from jax.sharding import PartitionSpec as P

F32, BF16, I32 = jnp.float32, jnp.bfloat16, jnp.int32
MESH = pl.DeviceIdType.MESH
GX_GY = ("gx", "gy")

WIDE_SLOTS = 4
THIN_SLOTS = 12
BLOCK = 256


def keys_of(index, first, count, axis):
    row = index - first
    place = lax.broadcasted_iota(I32, row.shape, axis)
    return jnp.where((row >= 0) & (row < count), row * 32 + place, -1)


def next_slot(keys, slot, axis=0):
    return jnp.max(jnp.where(keys < slot, keys, -1), axis=axis, keepdims=True)


def mark_of(values):
    return jnp.broadcast_to(values, (16, values.shape[1])).astype(BF16)


def wide_mark(slot):
    return jnp.where(slot < 0, 256, (slot >> 5) - 256).astype(F32)


def ids_of(first):
    return (lax.broadcasted_iota(I32, (16, 128), 0) + first).astype(F32).astype(BF16)


def one_hot(marks, chunk):
    one, zero = jnp.ones((16, 128), BF16), jnp.zeros((16, 128), BF16)
    hit = jnp.where(chunk == marks[0], one, zero)
    for mark in marks[1:]:
        hit = hit + jnp.where(chunk == mark, one, zero)
    return hit


def split_projection(table, weight):
    projected = jnp.dot(table, weight, preferred_element_type=F32).T
    high = projected.astype(BF16)
    low = (projected - high.astype(F32)).astype(BF16)
    return jnp.concatenate([high, low], axis=0)


def place_of(q, y_lo, y_hi, x):
    bits = ((x // 2) ^ (x % 2), y_hi ^ y_lo, x // 2, y_hi)
    return sum((8 >> ((d - q) % 4)) * bits[d] for d in range(4))


def find_kernel(rows_w, rows_t, wi, ti, wslot, tslot, wmore, tmore, left):
    gx, gy = lax.axis_index("gx"), lax.axis_index("gy")
    tables, _, bags = wi.shape
    first_w, first_t = (gx * 16 + gy) * rows_w, gy * rows_t

    most = jnp.full((1, 128), -1, I32)
    for t in range(tables):
        for b in range(bags // BLOCK):
            at = slice(b * BLOCK, (b + 1) * BLOCK)
            keys = keys_of(wi[t, :, at], first_w, rows_w, 0)
            slot = jnp.max(keys, axis=0, keepdims=True)
            for k in range(WIDE_SLOTS):
                wslot[t, k : k + 1, at] = wide_mark(slot)
                slot = next_slot(keys, slot)
            wmore[t, :, at] = slot
            for c in range(BLOCK // 128):
                most = jnp.maximum(most, slot[:, c * 128 : c * 128 + 128])
    left[0] = jnp.broadcast_to(most, (8, 128))

    thin_keys = keys_of(ti[...], first_t, rows_t, 1)
    slot = jnp.max(thin_keys, axis=1, keepdims=True)
    for k in range(THIN_SLOTS):
        tslot[:, k : k + 1, :] = slot >> 5
        slot = next_slot(thin_keys, slot, 1)
    tmore[...] = slot
    left[1] = jnp.broadcast_to(jnp.max(slot, axis=0), (8, 128))


def spill_kernel(
    wi, ti, wmore, tmore, left, wt, wp, tt, wextra, textra,
    wkeys, hits, proj, lines, low,
):
    gx, gy = lax.axis_index("gx"), lax.axis_index("gy")
    tables, _, bags = wi.shape
    rows_w, rows_t = wt.shape[1], tt.shape[2]
    first_w, first_t = (gx * 16 + gy) * rows_w, gy * rows_t
    blocks = bags // BLOCK
    wextra[...] = jnp.zeros_like(wextra)
    textra[...] = jnp.zeros_like(textra)
    wide_left, thin_left = jnp.max(left[0]), jnp.max(left[1])

    @pl.when(wide_left >= 0)
    def _():
        wkeys[...] = keys_of(wi[...], first_w, rows_w, 1)

        def table(t, _):
            @pl.when(jnp.max(wmore[t]) >= 0)
            def _():
                proj[...] = split_projection(wt[t], wp[t])

                def block(b, _):
                    at = pl.ds(pl.multiple_of(b * BLOCK, BLOCK), BLOCK)
                    top = jnp.max(wmore[t, :, at])

                    @pl.when(top >= 0)
                    def _():
                        hits[...] = jnp.zeros_like(hits)

                        def body(carry):
                            slot, _ = carry
                            for c in range(BLOCK // 128):
                                mark = mark_of(wide_mark(slot[:, c * 128 : c * 128 + 128]))
                                for r in range(rows_w // 16):
                                    spot = (slice(r * 16, r * 16 + 16), slice(c * 128, c * 128 + 128))
                                    hits[spot] = hits[spot] + one_hot([mark], ids_of(r * 16 - 256))
                            slot = next_slot(wkeys[t, :, at], slot)
                            return slot, jnp.max(slot)

                        lax.while_loop(lambda carry: carry[1] >= 0, body, (wmore[t, :, at], top))
                        both = jnp.dot(proj[...], hits[...], preferred_element_type=F32)
                        found = (both[:128] + both[128:]).T
                        for g in range(BLOCK // 128):
                            group = b * (BLOCK // 128) + g
                            y_lo, z = group // 8, group % 8
                            quarter = z // 2
                            step = [8 >> ((d - quarter + 4) % 4) for d in range(4)]
                            for y_hi in range(2):
                                crossed = (y_hi + y_lo) % 2
                                for x in range(4):
                                    place = step[0] * ((x // 2) ^ (x % 2)) + step[1] * crossed
                                    place = place + step[2] * (x // 2) + step[3] * y_hi
                                    place = quarter * 32 + place * 2 + z % 2
                                    for core in range(2):
                                        row = g * 128 + y_hi * 64 + x * 16 + core * 8
                                        wextra[t, core * 128 + place] = found[row : row + 8]

                    return 0

                lax.fori_loop(0, blocks, block, 0)

            return 0

        lax.fori_loop(0, tables, table, 0)

    @pl.when(thin_left >= 0)
    def _():
        groups = rows_t // 256

        def table(i, _):
            keys = keys_of(ti[i], first_t, rows_t, 0)
            slot = tmore[i]
            top = jnp.max(slot)

            @pl.when(top >= 0)
            def _():
                for g in range(groups):
                    lines[g * 32 : g * 32 + 32, :] = tt[i, :, g * 256 : g * 256 + 256]

                def body(carry):
                    slot, _ = carry
                    mark = mark_of(((slot >> 5) & 255).astype(F32))
                    for r in range(16):
                        low[r * 16 : r * 16 + 16, :] = one_hot([mark], ids_of(r * 16))
                    found = jnp.dot(lines[...], low[...], preferred_element_type=F32)
                    group = jnp.broadcast_to(slot >> 13, (32, 128))
                    total = textra[i]
                    for g in range(groups):
                        total = total + jnp.where(group == g, found[g * 32 : g * 32 + 32], 0.0)
                    textra[i] = total
                    slot = next_slot(keys, slot)
                    return slot, jnp.max(slot)

                lax.while_loop(lambda carry: carry[1] >= 0, body, (slot, top))

            return 0

        lax.fori_loop(0, ti.shape[0], table, 0)


def find(wide_index, thin_index, wide_table, wide_proj, thin_table):
    tw, _, bags = wide_index.shape
    tt, _, own_bags = thin_index.shape
    rows_w = wide_table.shape[1]
    wt, rows_t = thin_table.shape[1:]
    vmem = pl.BlockSpec(memory_space=pltpu.VMEM)
    params = pltpu.CompilerParams(vmem_limit_bytes=16 * 2**20)
    wslot, tslot, wmore, tmore, left = pl.pallas_call(
        functools.partial(find_kernel, rows_w, rows_t),
        in_specs=[vmem] * 2,
        out_specs=[vmem] * 5,
        out_shape=[
            jax.ShapeDtypeStruct((tw, WIDE_SLOTS, bags), F32),
            jax.ShapeDtypeStruct((tt, THIN_SLOTS, own_bags), I32),
            jax.ShapeDtypeStruct((tw, 1, bags), I32),
            jax.ShapeDtypeStruct((tt, 1, own_bags), I32),
            jax.ShapeDtypeStruct((2, 8, 128), I32),
        ],
        compiler_params=params,
        cost_estimate=pl.CostEstimate(flops=4 * 10**9, bytes_accessed=1 << 20, transcendentals=0),
    )(wide_index, thin_index)
    wextra, textra = pl.pallas_call(
        spill_kernel,
        in_specs=[vmem] * 8,
        out_specs=[vmem] * 2,
        out_shape=[
            jax.ShapeDtypeStruct((tw, bags // 8, 8, 128), F32),
            jax.ShapeDtypeStruct((tt, wt, own_bags), F32),
        ],
        scratch_shapes=[
            pltpu.VMEM(wide_index.shape, I32),
            pltpu.VMEM((rows_w, BLOCK), BF16),
            pltpu.VMEM((256, rows_w), BF16),
            pltpu.VMEM((rows_t // 256 * wt, 256), BF16),
            pltpu.VMEM((256, 128), BF16),
        ],
        compiler_params=params,
    )(wide_index, thin_index, wmore, tmore, left, wide_table, wide_proj, thin_table)
    return wslot, tslot, wextra, textra


def pool_kernel(
    wslot, tslot, wextra, textra, wt, wp, tt, pj, out,
    part, sums, th, r0, r1, r2, rm, r4, rz, rt,
    hs, hr, ss, sr, ms, mr, zs, zr, ts, tr, entered,
):
    gx, gy = lax.axis_index("gx"), lax.axis_index("gy")
    y_lo, z = gx // 8, gx % 8
    y_hi, x, core = gy // 8, (gy // 2) % 4, gy % 2
    every = range(4)

    def device(flip_lo, y_hi, x, core=core):
        return ((1 - y_lo if flip_lo else y_lo) * 8 + z, y_hi * 8 + x * 2 + core)

    moves = [
        (False, y_hi, x + 1 - 2 * (x % 2), (x // 2 + x % 2) % 2),
        (True, y_hi, x, (y_hi + y_lo) % 2),
        (False, y_hi, 3 - x, x // 2),
        (True, 1 - y_hi, x, y_hi),
    ]
    links = [device(*move[:3]) for move in moves]
    bits = [[moves[(q + k) % 4][3] for k in every] for q in every]
    partners = [[links[(q + k) % 4] for k in every] for q in every]
    corners = []
    for q in every:
        a, b = moves[(q + 2) % 4], moves[(q + 3) % 4]
        along_x, along_y = (a, b) if q % 2 == 0 else (b, a)
        corners.append(device(True, along_y[1], along_x[2]))
    other = device(False, y_hi, x, 1 - core)
    along_z = [None] + [(y_lo * 8 + (z + d) % 8, gy) for d in range(1, 8)]
    along_gy = [None] + [(gx, (gy + d) % 16) for d in range(1, 16)]

    barrier = pltpu.get_barrier_semaphore()
    peers = [other] + links + [along_z[1], along_z[7]]
    for peer in peers:
        pl.semaphore_signal(barrier, inc=1, device_id=peer, device_id_type=MESH)

    def relay(turn):
        if turn > 0:
            pl.semaphore_wait(entered.at[turn - 1], 2)
        if turn < 3:
            for peer in (along_z[1], along_z[7]):
                pl.semaphore_signal(entered.at[turn], inc=1, device_id=peer, device_id_type=MESH)

    sends = []

    def send(src, dst, s, r, to):
        copy = pltpu.make_async_remote_copy(
            src_ref=src, dst_ref=dst, send_sem=s, recv_sem=r, device_id=to, device_id_type=MESH
        )
        copy.start()
        sends.append(copy)
        return copy

    def wide_part(c):
        both_parts = split_projection(wt[c], wp[c])
        chunks = [ids_of(r * 16 - 256) for r in range(wt.shape[1] // 16)]
        for b in range(wslot.shape[2] // BLOCK):
            columns = []
            for g in range(BLOCK // 128):
                at = b * BLOCK + g * 128
                marks = [mark_of(wslot[c, k : k + 1, at : at + 128]) for k in range(WIDE_SLOTS)]
                columns.append(jnp.concatenate([one_hot(marks, chunk) for chunk in chunks], axis=0))
            hits = jnp.concatenate(columns, axis=1)
            both = jnp.dot(both_parts, hits, preferred_element_type=F32)
            found = (both[:128] + both[128:]).T
            for g in range(BLOCK // 128):
                g_lo, g_z = divmod(b * (BLOCK // 128) + g, 8)
                for g_hi in range(2):
                    for g_x in every:
                        place = place_of(g_z // 2, g_lo, g_hi, g_x)
                        for g_core in range(2):
                            row = g * 128 + g_hi * 64 + g_x * 16 + g_core * 8
                            spot = (c, g_core, g_z // 2, place, g_z % 2)
                            part[spot] = wextra[spot] + found[row : row + 8]

    def thin_table(i, _):
        groups = tt.shape[2] // 256
        lines = jnp.concatenate([tt[i, :, g * 256 : g * 256 + 256] for g in range(groups)], axis=0)
        chunks = [ids_of(r * 16) for r in range(16)]
        total = [textra[i, f * 8 : f * 8 + 8, :] for f in every]
        for pair in range(THIN_SLOTS // 2):
            slots = [tslot[i, pair * 2 + k : pair * 2 + k + 1, :] for k in range(2)]
            columns = []
            for slot in slots:
                mark = mark_of((slot & 255).astype(F32))
                columns.append(jnp.concatenate([one_hot([mark], chunk) for chunk in chunks], axis=0))
            low = jnp.concatenate(columns, axis=1)
            found = jnp.dot(lines, low, preferred_element_type=F32)
            for k in range(2):
                group = jnp.broadcast_to(slots[k] >> 8, (8, 128))
                picked = [jnp.zeros((8, 128), F32)] * 4
                for g in range(groups):
                    same = group == g
                    for f in every:
                        row = g * 32 + f * 8
                        piece = found[row : row + 8, k * 128 : k * 128 + 128]
                        picked[f] = jnp.where(same, piece, picked[f])
                total = [a + b for a, b in zip(total, picked)]
        for f in every:
            sums[pl.ds(pl.multiple_of(i * 32 + f * 8, 8), 8), :] = total[f]
        return 0

    halves, first, second, third, lasts = {}, {}, {}, {}, {}

    def send_half(c):
        halves[c] = send(part.at[c, 1 - core], r0.at[c], hs.at[c], hr.at[c], other)

    def send_first(c):
        halves[c].wait_recv()
        for turn in range(2):
            for q in every:
                half = pl.ds((1 - bits[q][0] if turn == 0 else bits[q][0]) * 8, 8)
                part[c, core, q, half] = part[c, core, q, half] + r0[c, q, half]
                if turn == 0:
                    first[c, q] = send(
                        part.at[c, core, q, half], r1.at[c, q], ss.at[0, c, q], sr.at[0, c, q],
                        partners[q][0],
                    )

    def send_second(c):
        for q in every:
            first[c, q].wait_recv()
            side = 1 - bits[q][1]
            half = pl.ds(side * 4, 4)
            r1[c, q, half] = r1[c, q, half] + part[c, core, q, pl.ds(bits[q][0] * 8 + side * 4, 4)]
            second[c, q] = send(
                r1.at[c, q, half], r2.at[c, q], ss.at[1, c, q], sr.at[1, c, q], partners[q][1]
            )
        for q in every:
            side = bits[q][1]
            half = pl.ds(side * 4, 4)
            r1[c, q, half] = r1[c, q, half] + part[c, core, q, pl.ds(bits[q][0] * 8 + side * 4, 4)]

    def send_third(c):
        for q in every:
            second[c, q].wait_recv()
            b1, b2, b3 = bits[q][1:]
            ways = [
                (1 - b2, 1 - b3, corners[q]),
                (1 - b2, b3, partners[q][2]),
                (b2, 1 - b3, partners[q][3]),
            ]
            for j, (i2, i3, to) in enumerate(ways):
                here = i2 * 2 + i3
                r2[c, q, here] = r2[c, q, here] + r1[c, q, b1 * 4 + here]
                third[c, q, j] = send(
                    r2.at[c, q, here], rm.at[c, q, j], ms.at[c, q, j], mr.at[c, q, j], to
                )

    def send_last(c):
        for q in every:
            b1, b2, b3 = bits[q][1:]
            here = b2 * 2 + b3
            total = r2[c, q, here] + r1[c, q, b1 * 4 + here]
            for j in (1, 2, 0):
                third[c, q, j].wait_recv()
                total = total + rm[c, q, j]
            r4[c, q * 2 : q * 2 + 2] = total
        for d in (4, 3, 5, 2, 6, 1, 7):
            lasts[c, d] = send(
                r4.at[c, (z + d) % 8], rz.at[d, c], zs.at[d, c], zr.at[d, c], along_z[d]
            )

    def thin_tables(begin, end):
        lax.fori_loop(begin, end, thin_table, 0)

    wide_part(0)
    pl.semaphore_wait(barrier, len(peers))
    send_half(0)
    relay(0)
    wide_part(1)
    send_half(1)
    send_first(0)
    wide_part(2)
    send_half(2)
    send_first(1)
    wide_part(3)
    send_half(3)
    relay(1)
    thin_tables(0, 1)
    send_first(2)
    thin_tables(1, 2)
    send_second(0)
    send_first(3)
    relay(2)
    thin_tables(2, 3)
    send_second(1)
    thin_tables(3, 4)
    send_third(0)
    send_second(2)
    relay(3)
    thin_tables(4, 5)
    send_second(3)
    send_third(1)
    thin_tables(5, 6)
    send_last(0)
    send_third(2)
    thin_tables(6, 7)
    send_third(3)
    thin_tables(7, 8)
    for h in range(2):
        th[h] = sums[h * 128 : h * 128 + 128, :].T.reshape(16, 8, 128)
    thins = []
    for d in range(1, 16):
        thins.append(send(th.at[:, along_gy[d][1]], rt.at[d], ts.at[d], tr.at[d], along_gy[d]))
    send_last(1)
    send_last(2)
    send_last(3)

    for copy in thins:
        copy.wait_recv()
    pooled = th[:, gy]
    for d in range(1, 16):
        pooled = pooled + rt[d]
    group = lax.broadcasted_iota(I32, (8, 128), 1) // 32
    for h in range(2):
        rows = jnp.concatenate([jnp.where(group == g, pooled[h], 0.0) for g in every], axis=0)
        projected = jnp.dot(
            rows, pj[h].astype(F32), preferred_element_type=F32, precision=lax.Precision.HIGHEST
        )
        for g in every:
            at = 512 + (h * 4 + g) * 128
            out[:, at : at + 128] = projected[g * 8 : g * 8 + 8]

    for c in every:
        total = r4[c, z]
        for d in (1, 7, 2, 6, 3, 5, 4):
            lasts[c, d].wait_recv()
            total = total + rz[d, c]
        out[:, c * 128 : c * 128 + 128] = total
    for copy in sends:
        copy.wait_send()


def pool(wslot, tslot, wextra, textra, wide_table, wide_proj, thin_table, thin_proj):
    vmem = pl.BlockSpec(memory_space=pltpu.VMEM)
    dma = pltpu.SemaphoreType.DMA
    return pl.pallas_call(
        pool_kernel,
        in_specs=[vmem] * 8,
        out_specs=vmem,
        out_shape=jax.ShapeDtypeStruct((8, 1536), F32),
        scratch_shapes=[
            pltpu.VMEM((4, 2, 4, 16, 2, 8, 128), F32),
            pltpu.VMEM((256, 128), F32),
            pltpu.VMEM((2, 16, 8, 128), F32),
            pltpu.VMEM((4, 4, 16, 2, 8, 128), F32),
            pltpu.VMEM((4, 4, 8, 2, 8, 128), F32),
            pltpu.VMEM((4, 4, 4, 2, 8, 128), F32),
            pltpu.VMEM((4, 4, 3, 2, 8, 128), F32),
            pltpu.VMEM((4, 8, 8, 128), F32),
            pltpu.VMEM((8, 4, 8, 128), F32),
            pltpu.VMEM((16, 2, 8, 128), F32),
            dma((4,)),
            dma((4,)),
            dma((2, 4, 4)),
            dma((2, 4, 4)),
            dma((4, 4, 3)),
            dma((4, 4, 3)),
            dma((8, 4)),
            dma((8, 4)),
            dma((16,)),
            dma((16,)),
            pltpu.SemaphoreType.REGULAR((3,)),
        ],
        compiler_params=pltpu.CompilerParams(
            collective_id=0, has_side_effects=True, vmem_limit_bytes=24 * 2**20
        ),
    )(
        wslot, tslot, wextra.reshape(4, 2, 4, 16, 2, 8, 128), textra,
        wide_table, wide_proj, thin_table, thin_proj.reshape(2, 128, 128),
    )


def local(wide_index, wide_table, wide_proj, thin_index, thin_table, thin_proj):
    wslot, tslot, wextra, textra = find(wide_index, thin_index, wide_table, wide_proj, thin_table)
    out = pool(wslot, tslot, wextra, textra, wide_table, wide_proj, thin_table, thin_proj)
    return out[:, :512], out[:, 512:]


def solution(mesh):
    placed = (P(), P(None, GX_GY, None), P(), P(None, None, "gx"), P(None, None, "gy"), P())
    return jax.shard_map(
        local,
        mesh=mesh,
        in_specs=placed,
        out_specs=(P(GX_GY, None), P(GX_GY, None)),
        check_vma=False,
    )
```

```python
import functools

import jax
import jax.numpy as jnp
from jax import lax
from jax.experimental import pallas as pl
from jax.experimental.pallas import tpu as pltpu
from jax.sharding import PartitionSpec as P

F32, BF16, I32 = jnp.float32, jnp.bfloat16, jnp.int32
MESH = pl.DeviceIdType.MESH
GX_GY = ("gx", "gy")

WIDE_SLOTS = 4
THIN_SLOTS = 12
BLOCK = 256


def keys_of(index, first, count, axis):
    row = index - first
    place = lax.broadcasted_iota(I32, row.shape, axis)
    return jnp.where((row >= 0) & (row < count), row * 32 + place, -1)


def next_slot(keys, slot, axis=0):
    return jnp.max(jnp.where(keys < slot, keys, -1), axis=axis, keepdims=True)


def mark_of(values):
    return jnp.broadcast_to(values, (16, values.shape[1])).astype(BF16)


def wide_mark(slot):
    return jnp.where(slot < 0, 256, (slot >> 5) - 256).astype(F32)


def ids_of(first):
    return (lax.broadcasted_iota(I32, (16, 128), 0) + first).astype(F32).astype(BF16)


def one_hot(marks, chunk):
    one, zero = jnp.ones((16, 128), BF16), jnp.zeros((16, 128), BF16)
    hit = jnp.where(chunk == marks[0], one, zero)
    for mark in marks[1:]:
        hit = hit + jnp.where(chunk == mark, one, zero)
    return hit


def split_projection(table, weight):
    projected = jnp.dot(table, weight, preferred_element_type=F32).T
    high = projected.astype(BF16)
    low = (projected - high.astype(F32)).astype(BF16)
    return jnp.concatenate([high, low], axis=0)


def place_of(q, y_lo, y_hi, x):
    bits = ((x // 2) ^ (x % 2), y_hi ^ y_lo, x // 2, y_hi)
    return sum((8 >> ((d - q) % 4)) * bits[d] for d in range(4))


def find_kernel(rows_w, rows_t, wi, ti, wslot, tslot, wmore, tmore, left):
    gx, gy = lax.axis_index("gx"), lax.axis_index("gy")
    tables, _, bags = wi.shape
    first_w, first_t = (gx * 16 + gy) * rows_w, gy * rows_t

    most = jnp.full((1, 128), -1, I32)
    for t in range(tables):
        for b in range(bags // BLOCK):
            at = slice(b * BLOCK, (b + 1) * BLOCK)
            keys = keys_of(wi[t, :, at], first_w, rows_w, 0)
            slot = jnp.max(keys, axis=0, keepdims=True)
            for k in range(WIDE_SLOTS):
                wslot[t, k : k + 1, at] = wide_mark(slot)
                slot = next_slot(keys, slot)
            wmore[t, :, at] = slot
            for c in range(BLOCK // 128):
                most = jnp.maximum(most, slot[:, c * 128 : c * 128 + 128])
    left[0] = jnp.broadcast_to(most, (8, 128))

    thin_keys = keys_of(ti[...], first_t, rows_t, 1)
    slot = jnp.max(thin_keys, axis=1, keepdims=True)
    for k in range(THIN_SLOTS):
        tslot[:, k : k + 1, :] = slot >> 5
        slot = next_slot(thin_keys, slot, 1)
    tmore[...] = slot
    left[1] = jnp.broadcast_to(jnp.max(slot, axis=0), (8, 128))


def spill_kernel(
    wi, ti, wmore, tmore, left, wt, wp, tt, pj, wextra, textra,
    wkeys, hits, proj, lines, low,
):
    gx, gy = lax.axis_index("gx"), lax.axis_index("gy")
    tables, _, bags = wi.shape
    rows_w, rows_t = wt.shape[1], tt.shape[2]
    first_w, first_t = (gx * 16 + gy) * rows_w, gy * rows_t
    blocks = bags // BLOCK
    wextra[...] = jnp.zeros_like(wextra)
    textra[...] = jnp.zeros_like(textra)
    wide_left, thin_left = jnp.max(left[0]), jnp.max(left[1])

    @pl.when(wide_left >= 0)
    def _():
        wkeys[...] = keys_of(wi[...], first_w, rows_w, 1)

        def table(t, _):
            @pl.when(jnp.max(wmore[t]) >= 0)
            def _():
                proj[...] = split_projection(wt[t], wp[t])

                def block(b, _):
                    at = pl.ds(pl.multiple_of(b * BLOCK, BLOCK), BLOCK)
                    top = jnp.max(wmore[t, :, at])

                    @pl.when(top >= 0)
                    def _():
                        hits[...] = jnp.zeros_like(hits)

                        def body(carry):
                            slot, _ = carry
                            for c in range(BLOCK // 128):
                                mark = mark_of(wide_mark(slot[:, c * 128 : c * 128 + 128]))
                                for r in range(rows_w // 16):
                                    spot = (slice(r * 16, r * 16 + 16), slice(c * 128, c * 128 + 128))
                                    hits[spot] = hits[spot] + one_hot([mark], ids_of(r * 16 - 256))
                            slot = next_slot(wkeys[t, :, at], slot)
                            return slot, jnp.max(slot)

                        lax.while_loop(lambda carry: carry[1] >= 0, body, (wmore[t, :, at], top))
                        both = jnp.dot(proj[...], hits[...], preferred_element_type=F32)
                        found = (both[:128] + both[128:]).T
                        for g in range(BLOCK // 128):
                            group = b * (BLOCK // 128) + g
                            y_lo, z = group // 8, group % 8
                            quarter = z // 2
                            step = [8 >> ((d - quarter + 4) % 4) for d in range(4)]
                            for y_hi in range(2):
                                crossed = (y_hi + y_lo) % 2
                                for x in range(4):
                                    place = step[0] * ((x // 2) ^ (x % 2)) + step[1] * crossed
                                    place = place + step[2] * (x // 2) + step[3] * y_hi
                                    place = quarter * 32 + place * 2 + z % 2
                                    for core in range(2):
                                        row = g * 128 + y_hi * 64 + x * 16 + core * 8
                                        wextra[t, core * 128 + place] = found[row : row + 8]

                    return 0

                lax.fori_loop(0, blocks, block, 0)

            return 0

        lax.fori_loop(0, tables, table, 0)

    @pl.when(thin_left >= 0)
    def _():
        groups = rows_t // 256

        def table(i, _):
            keys = keys_of(ti[i], first_t, rows_t, 0)
            slot = tmore[i]
            top = jnp.max(slot)

            @pl.when(top >= 0)
            def _():
                for g in range(groups):
                    lines[g * 32 : g * 32 + 32, :] = tt[i, :, g * 256 : g * 256 + 256]

                def body(carry):
                    slot, _ = carry
                    mark = mark_of(((slot >> 5) & 255).astype(F32))
                    for r in range(16):
                        low[r * 16 : r * 16 + 16, :] = one_hot([mark], ids_of(r * 16))
                    found = jnp.dot(lines[...], low[...], preferred_element_type=F32)
                    group = jnp.broadcast_to(slot >> 13, (32, 128))
                    total = textra[i]
                    for g in range(groups):
                        total = total + jnp.where(group == g, found[g * 32 : g * 32 + 32], 0.0)
                    textra[i] = total
                    slot = next_slot(keys, slot)
                    return slot, jnp.max(slot)

                lax.while_loop(lambda carry: carry[1] >= 0, body, (slot, top))

            return 0

        lax.fori_loop(0, ti.shape[0], table, 0)


def find(wide_index, thin_index, wide_table, wide_proj, thin_table, thin_proj):
    tw, _, bags = wide_index.shape
    tt, _, own_bags = thin_index.shape
    rows_w = wide_table.shape[1]
    wt, rows_t = thin_table.shape[1:]
    vmem = pl.BlockSpec(memory_space=pltpu.VMEM)
    params = pltpu.CompilerParams(vmem_limit_bytes=16 * 2**20)
    wslot, tslot, wmore, tmore, left = pl.pallas_call(
        functools.partial(find_kernel, rows_w, rows_t),
        in_specs=[vmem] * 2,
        out_specs=[vmem] * 5,
        out_shape=[
            jax.ShapeDtypeStruct((tw, WIDE_SLOTS, bags), F32),
            jax.ShapeDtypeStruct((tt, THIN_SLOTS, own_bags), I32),
            jax.ShapeDtypeStruct((tw, 1, bags), I32),
            jax.ShapeDtypeStruct((tt, 1, own_bags), I32),
            jax.ShapeDtypeStruct((2, 8, 128), I32),
        ],
        compiler_params=params,
        cost_estimate=pl.CostEstimate(flops=4 * 10**9, bytes_accessed=1 << 20, transcendentals=0),
    )(wide_index, thin_index)
    wextra, textra = pl.pallas_call(
        spill_kernel,
        in_specs=[vmem] * 9,
        out_specs=[vmem] * 2,
        out_shape=[
            jax.ShapeDtypeStruct((tw, bags // 8, 8, 128), F32),
            jax.ShapeDtypeStruct((tt, wt, own_bags), F32),
        ],
        scratch_shapes=[
            pltpu.VMEM(wide_index.shape, I32),
            pltpu.VMEM((rows_w, BLOCK), BF16),
            pltpu.VMEM((256, rows_w), BF16),
            pltpu.VMEM((rows_t // 256 * wt, 256), BF16),
            pltpu.VMEM((256, 128), BF16),
        ],
        compiler_params=params,
    )(wide_index, thin_index, wmore, tmore, left, wide_table, wide_proj, thin_table, thin_proj)
    return wslot, tslot, wextra, textra


def pool_kernel(
    wslot, tslot, wextra, textra, wt, wp, tt, pj, out,
    part, sums, th, r0, r1, r2, rm, r4, rz, rt,
    hs, hr, ss, sr, ms, mr, zs, zr, ts, tr, entered,
):
    gx, gy = lax.axis_index("gx"), lax.axis_index("gy")
    y_lo, z = gx // 8, gx % 8
    y_hi, x, core = gy // 8, (gy // 2) % 4, gy % 2
    every = range(4)

    def device(flip_lo, y_hi, x, core=core):
        return ((1 - y_lo if flip_lo else y_lo) * 8 + z, y_hi * 8 + x * 2 + core)

    moves = [
        (False, y_hi, x + 1 - 2 * (x % 2), (x // 2 + x % 2) % 2),
        (True, y_hi, x, (y_hi + y_lo) % 2),
        (False, y_hi, 3 - x, x // 2),
        (True, 1 - y_hi, x, y_hi),
    ]
    links = [device(*move[:3]) for move in moves]
    bits = [[moves[(q + k) % 4][3] for k in every] for q in every]
    partners = [[links[(q + k) % 4] for k in every] for q in every]
    corners = []
    for q in every:
        a, b = moves[(q + 2) % 4], moves[(q + 3) % 4]
        along_x, along_y = (a, b) if q % 2 == 0 else (b, a)
        corners.append(device(True, along_y[1], along_x[2]))
    other = device(False, y_hi, x, 1 - core)
    along_z = [None] + [(y_lo * 8 + (z + d) % 8, gy) for d in range(1, 8)]
    along_gy = [None] + [(gx, (gy + d) % 16) for d in range(1, 16)]

    barrier = pltpu.get_barrier_semaphore()
    peers = [other] + links + [along_z[1], along_z[7]]
    for peer in peers:
        pl.semaphore_signal(barrier, inc=1, device_id=peer, device_id_type=MESH)

    def relay(turn):
        if turn > 0:
            pl.semaphore_wait(entered.at[turn - 1], 2)
        if turn < 3:
            for peer in (along_z[1], along_z[7]):
                pl.semaphore_signal(entered.at[turn], inc=1, device_id=peer, device_id_type=MESH)

    sends = []

    def send(src, dst, s, r, to):
        copy = pltpu.make_async_remote_copy(
            src_ref=src, dst_ref=dst, send_sem=s, recv_sem=r, device_id=to, device_id_type=MESH
        )
        copy.start()
        sends.append(copy)
        return copy

    def wide_part(c):
        both_parts = split_projection(wt[c], wp[c])
        chunks = [ids_of(r * 16 - 256) for r in range(wt.shape[1] // 16)]
        for b in range(wslot.shape[2] // BLOCK):
            columns = []
            for g in range(BLOCK // 128):
                at = b * BLOCK + g * 128
                marks = [mark_of(wslot[c, k : k + 1, at : at + 128]) for k in range(WIDE_SLOTS)]
                columns.append(jnp.concatenate([one_hot(marks, chunk) for chunk in chunks], axis=0))
            hits = jnp.concatenate(columns, axis=1)
            both = jnp.dot(both_parts, hits, preferred_element_type=F32)
            found = (both[:128] + both[128:]).T
            for g in range(BLOCK // 128):
                g_lo, g_z = divmod(b * (BLOCK // 128) + g, 8)
                for g_hi in range(2):
                    for g_x in every:
                        place = place_of(g_z // 2, g_lo, g_hi, g_x)
                        for g_core in range(2):
                            row = g * 128 + g_hi * 64 + g_x * 16 + g_core * 8
                            spot = (c, g_core, g_z // 2, place, g_z % 2)
                            part[spot] = wextra[spot] + found[row : row + 8]

    def thin_table(i, _):
        groups = tt.shape[2] // 256
        lines = jnp.concatenate([tt[i, :, g * 256 : g * 256 + 256] for g in range(groups)], axis=0)
        chunks = [ids_of(r * 16) for r in range(16)]
        total = [textra[i, f * 8 : f * 8 + 8, :] for f in every]
        for pair in range(THIN_SLOTS // 2):
            slots = [tslot[i, pair * 2 + k : pair * 2 + k + 1, :] for k in range(2)]
            columns = []
            for slot in slots:
                mark = mark_of((slot & 255).astype(F32))
                columns.append(jnp.concatenate([one_hot([mark], chunk) for chunk in chunks], axis=0))
            low = jnp.concatenate(columns, axis=1)
            found = jnp.dot(lines, low, preferred_element_type=F32)
            for k in range(2):
                group = jnp.broadcast_to(slots[k] >> 8, (8, 128))
                picked = [jnp.zeros((8, 128), F32)] * 4
                for g in range(groups):
                    same = group == g
                    for f in every:
                        row = g * 32 + f * 8
                        piece = found[row : row + 8, k * 128 : k * 128 + 128]
                        picked[f] = jnp.where(same, piece, picked[f])
                total = [a + b for a, b in zip(total, picked)]
        for f in every:
            sums[pl.ds(pl.multiple_of(i * 32 + f * 8, 8), 8), :] = total[f]
        return 0

    halves, first, second, third, lasts = {}, {}, {}, {}, {}

    def send_half(c):
        halves[c] = send(part.at[c, 1 - core], r0.at[c], hs.at[c], hr.at[c], other)

    def send_first(c):
        halves[c].wait_recv()
        for turn in range(2):
            for q in every:
                half = pl.ds((1 - bits[q][0] if turn == 0 else bits[q][0]) * 8, 8)
                part[c, core, q, half] = part[c, core, q, half] + r0[c, q, half]
                if turn == 0:
                    first[c, q] = send(
                        part.at[c, core, q, half], r1.at[c, q], ss.at[0, c, q], sr.at[0, c, q],
                        partners[q][0],
                    )

    def send_second(c):
        for q in every:
            first[c, q].wait_recv()
            side = 1 - bits[q][1]
            half = pl.ds(side * 4, 4)
            r1[c, q, half] = r1[c, q, half] + part[c, core, q, pl.ds(bits[q][0] * 8 + side * 4, 4)]
            second[c, q] = send(
                r1.at[c, q, half], r2.at[c, q], ss.at[1, c, q], sr.at[1, c, q], partners[q][1]
            )
        for q in every:
            side = bits[q][1]
            half = pl.ds(side * 4, 4)
            r1[c, q, half] = r1[c, q, half] + part[c, core, q, pl.ds(bits[q][0] * 8 + side * 4, 4)]

    def send_third(c):
        for q in every:
            second[c, q].wait_recv()
            b1, b2, b3 = bits[q][1:]
            ways = [
                (1 - b2, 1 - b3, corners[q]),
                (1 - b2, b3, partners[q][2]),
                (b2, 1 - b3, partners[q][3]),
            ]
            for j, (i2, i3, to) in enumerate(ways):
                here = i2 * 2 + i3
                r2[c, q, here] = r2[c, q, here] + r1[c, q, b1 * 4 + here]
                third[c, q, j] = send(
                    r2.at[c, q, here], rm.at[c, q, j], ms.at[c, q, j], mr.at[c, q, j], to
                )

    def send_last(c):
        for q in every:
            b1, b2, b3 = bits[q][1:]
            here = b2 * 2 + b3
            total = r2[c, q, here] + r1[c, q, b1 * 4 + here]
            for j in (1, 2, 0):
                third[c, q, j].wait_recv()
                total = total + rm[c, q, j]
            r4[c, q * 2 : q * 2 + 2] = total
        for d in (4, 3, 5, 2, 6, 1, 7):
            lasts[c, d] = send(
                r4.at[c, (z + d) % 8], rz.at[d, c], zs.at[d, c], zr.at[d, c], along_z[d]
            )

    def thin_tables(begin, end):
        lax.fori_loop(begin, end, thin_table, 0)

    wide_part(0)
    pl.semaphore_wait(barrier, len(peers))
    send_half(0)
    relay(0)
    wide_part(1)
    send_half(1)
    send_first(0)
    wide_part(2)
    send_half(2)
    send_first(1)
    wide_part(3)
    send_half(3)
    relay(1)
    thin_tables(0, 1)
    send_first(2)
    thin_tables(1, 2)
    send_second(0)
    send_first(3)
    relay(2)
    thin_tables(2, 3)
    send_second(1)
    thin_tables(3, 4)
    send_third(0)
    send_second(2)
    relay(3)
    thin_tables(4, 5)
    send_second(3)
    send_third(1)
    thin_tables(5, 6)
    send_last(0)
    send_third(2)
    thin_tables(6, 7)
    send_third(3)
    thin_tables(7, 8)
    for h in range(2):
        th[h] = sums[h * 128 : h * 128 + 128, :].T.reshape(16, 8, 128)
    thins = []
    for d in range(1, 16):
        thins.append(send(th.at[:, along_gy[d][1]], rt.at[d], ts.at[d], tr.at[d], along_gy[d]))
    send_last(1)
    send_last(2)
    send_last(3)

    for copy in thins:
        copy.wait_recv()
    pooled = th[:, gy]
    for d in range(1, 16):
        pooled = pooled + rt[d]
    group = lax.broadcasted_iota(I32, (8, 128), 1) // 32
    for h in range(2):
        rows = jnp.concatenate([jnp.where(group == g, pooled[h], 0.0) for g in every], axis=0)
        projected = jnp.dot(
            rows, pj[h].astype(F32), preferred_element_type=F32, precision=lax.Precision.HIGHEST
        )
        for g in every:
            at = 512 + (h * 4 + g) * 128
            out[:, at : at + 128] = projected[g * 8 : g * 8 + 8]

    for c in every:
        total = r4[c, z]
        for d in (1, 7, 2, 6, 3, 5, 4):
            lasts[c, d].wait_recv()
            total = total + rz[d, c]
        out[:, c * 128 : c * 128 + 128] = total
    for copy in sends:
        copy.wait_send()


def pool(wslot, tslot, wextra, textra, wide_table, wide_proj, thin_table, thin_proj):
    vmem = pl.BlockSpec(memory_space=pltpu.VMEM)
    dma = pltpu.SemaphoreType.DMA
    return pl.pallas_call(
        pool_kernel,
        in_specs=[vmem] * 8,
        out_specs=vmem,
        out_shape=jax.ShapeDtypeStruct((8, 1536), F32),
        scratch_shapes=[
            pltpu.VMEM((4, 2, 4, 16, 2, 8, 128), F32),
            pltpu.VMEM((256, 128), F32),
            pltpu.VMEM((2, 16, 8, 128), F32),
            pltpu.VMEM((4, 4, 16, 2, 8, 128), F32),
            pltpu.VMEM((4, 4, 8, 2, 8, 128), F32),
            pltpu.VMEM((4, 4, 4, 2, 8, 128), F32),
            pltpu.VMEM((4, 4, 3, 2, 8, 128), F32),
            pltpu.VMEM((4, 8, 8, 128), F32),
            pltpu.VMEM((8, 4, 8, 128), F32),
            pltpu.VMEM((16, 2, 8, 128), F32),
            dma((4,)),
            dma((4,)),
            dma((2, 4, 4)),
            dma((2, 4, 4)),
            dma((4, 4, 3)),
            dma((4, 4, 3)),
            dma((8, 4)),
            dma((8, 4)),
            dma((16,)),
            dma((16,)),
            pltpu.SemaphoreType.REGULAR((3,)),
        ],
        compiler_params=pltpu.CompilerParams(
            collective_id=0, has_side_effects=True, vmem_limit_bytes=24 * 2**20
        ),
    )(
        wslot, tslot, wextra.reshape(4, 2, 4, 16, 2, 8, 128), textra,
        wide_table, wide_proj, thin_table, thin_proj,
    )


def local(wide_index, wide_table, wide_proj, thin_index, thin_table, thin_proj):
    thin_proj = thin_proj.reshape(2, 128, 128)
    wslot, tslot, wextra, textra = find(wide_index, thin_index, wide_table, wide_proj, thin_table, thin_proj)
    out = pool(wslot, tslot, wextra, textra, wide_table, wide_proj, thin_table, thin_proj)
    return out[:, :512], out[:, 512:]


def solution(mesh):
    placed = (P(), P(None, GX_GY, None), P(), P(None, None, "gx"), P(None, None, "gy"), P())
    return jax.shard_map(
        local,
        mesh=mesh,
        in_specs=placed,
        out_specs=(P(GX_GY, None), P(GX_GY, None)),
        check_vma=False,
    )
```
